32 devices in a mesh: gx: 4 (over y, core), gy: 8 (over z, x).
Axes of the slice: x: 2, y: 2, z: 4, core: 2. Of those that a mesh axis runs over, the one named last changes fastest.
Arguments:
- populations: float32 [19, 16, 64, 128], P(None, 'gx', 'gy'), may hold values from 0.004 to 0.8, as said below
- solid: int32 [16, 64, 128], P('gx', 'gy'), may hold values 0 or 1
- base_cell: int32 [3, 4, 8, 2, 768], P(None, 'gx', 'gy'), may hold values from 0 to 127, as said below
- offset: float32 [3, 4, 8, 2, 768], P(None, 'gx', 'gy'), may hold values from 0 to 1
- rest_displacement: float32 [3, 4, 8, 2, 768], P(None, 'gx', 'gy'), may hold values from 0 to 1
- stiffness: float32 [4, 8, 2], P('gx', 'gy'), may hold values from 0.006380062 to 0.063800626
- occupied: int32 [4, 8, 2], P('gx', 'gy'), may hold values from 0 to 1, as said below
- triangles: int32 [1280, 3], replicated, may hold values from 0 to 641, as said below
Outputs:
- populations_out: float32 [19, 16, 64, 128], P(None, 'gx', 'gy')
- offset_out: float32 [3, 4, 8, 2, 768], P(None, 'gx', 'gy')
The draws below stay inside these ranges and needn't reach their ends.
Inputs may be any that keep to these rules, and one draw needn't show every extreme that they name: `populations`: every entry is positive. `base_cell`: component 0 of a vertex stored at index i of gx lies in [i * 4, (i + 1) * 4), component 1 of one stored at index j of gy lies in [j * 8, (j + 1) * 8), component 2 lies below 128. The occupied slots of a device come first; each device has at least one, and some device has all 2. `triangles`: each row holds three different vertex numbers below 642.
All inputs are finite; a program needn't handle non-finite values. No bound on the sum of `solid` on one device may be relied on, other than what follows from the above.
Results may differ from the reference program's by a relative error of at most 0.0001.
Values sent between devices are 32-bit elements; how exact they have to be, the bound alone decides.
A program may use at most 64 MiB of HBM per device.

```python
import math
import jax
import jax.numpy as jnp

CX = 4
CY = 8
CZ = 128
MEMBRANE_SLOTS = 2
VERTS = 642
PADDED_VERTICES = 768
TRIS = 1280
SUBSTEPS = 3
NX = 16
NY = 64
NZ = 128
N_GX = 4
N_GY = 8


DRAW_VELOCITIES = [[0, 0, 0], [1, 0, 0], [-1, 0, 0], [0, 1, 0], [0, -1, 0], [0, 0, 1], [0, 0, -1], [1, 1, 0], [-1, -1, 0], [1, -1, 0], [-1, 1, 0], [1, 0, 1], [-1, 0, -1], [1, 0, -1], [-1, 0, 1], [0, 1, 1], [0, -1, -1], [0, 1, -1], [0, -1, 1]]


DRAW_WEIGHTS = [1.0 / 3.0] + [1.0 / 18.0] * 6 + [1.0 / 36.0] * 12


def draw_populations(key, part):
    key_flow, key_noise = jax.random.split(jax.random.fold_in(key, 11))
    flow = jax.random.uniform(key_flow, (3, NX, NY, NZ), jnp.float32, -0.1, 0.1)
    noise = jax.random.uniform(key_noise, (19, NX, NY, NZ), jnp.float32, 0.7, 1.3)
    halo_layers = []
    for lattice_direction in range(19):
        vector = DRAW_VELOCITIES[lattice_direction]
        along = vector[0] * flow[0] + vector[1] * flow[1] + vector[2] * flow[2]
        halo_layers.append(DRAW_WEIGHTS[lattice_direction] * (1.0 + 3.0 * along) * noise[lattice_direction])
    return jnp.stack(halo_layers)


def draw_base_cell(key, part):
    key_x, key_y, key_z = jax.random.split(jax.random.fold_in(key, 23), 3)
    domain_extent = (N_GX, N_GY, MEMBRANE_SLOTS, PADDED_VERTICES)
    start_x = (jnp.arange(N_GX, dtype=jnp.int32) * CX).reshape(N_GX, 1, 1, 1)
    start_y = (jnp.arange(N_GY, dtype=jnp.int32) * CY).reshape(1, N_GY, 1, 1)
    cell_x = jax.random.randint(key_x, domain_extent, 0, CX, dtype=jnp.int32) + start_x
    cell_y = jax.random.randint(key_y, domain_extent, 0, CY, dtype=jnp.int32) + start_y
    cell_z = jax.random.randint(key_z, domain_extent, 0, CZ, dtype=jnp.int32)
    return jnp.stack([cell_x, cell_y, cell_z])


def draw_occupied(key, part):
    key_level, key_full = jax.random.split(jax.random.fold_in(key, 37))
    level = jax.random.randint(key_level, (N_GX, N_GY), 1, MEMBRANE_SLOTS + 1, dtype=jnp.int32)
    chosen = jax.random.randint(key_full, (), 0, N_GX * N_GY, dtype=jnp.int32)
    device_number = jnp.arange(N_GX * N_GY, dtype=jnp.int32).reshape(N_GX, N_GY)
    level = jnp.where(device_number == chosen, MEMBRANE_SLOTS, level)
    slot_number = jnp.arange(MEMBRANE_SLOTS, dtype=jnp.int32)[None, None, :]
    return (slot_number < level[:, :, None]).astype(jnp.int32)


def draw_triangles(key, part):
    key_first, key_near, distant_key = jax.random.split(jax.random.fold_in(key, 53), 3)
    half = VERTS // 2
    first = jax.random.randint(key_first, (TRIS,), 0, VERTS, dtype=jnp.int32)
    near = jax.random.randint(key_near, (TRIS,), 1, half, dtype=jnp.int32)
    far = jax.random.randint(distant_key, (TRIS,), half, VERTS, dtype=jnp.int32)
    return jnp.stack([first, (first + near) % VERTS, (first + far) % VERTS], axis=1)


def touch_ends(entries, rng, smallest, high):
    place = [jax.random.randint(jax.random.fold_in(rng, axis), (), 0, length) for axis, length in enumerate(entries.shape)]
    main_axis = entries.shape.index(max(entries.shape))
    beside = place[:main_axis] + [(place[main_axis] + 1) % entries.shape[main_axis]] + place[main_axis + 1:]
    return entries.at[tuple(place)].set(smallest).at[tuple(beside)].set(high)


def block_levels(own_key, shape, cuts, low, top_value):
    def one(dim, blocks):
        steps = jax.random.uniform(jax.random.fold_in(jax.random.fold_in(own_key, 6), dim), (blocks,), jnp.float32, low / len(cuts), top_value / len(cuts))
        return jnp.repeat(jnp.exp(steps), shape[dim] // blocks).reshape((-1,) + (1,) * (len(shape) - dim - 1))

    factor_of = one(*cuts[0])
    for cut in cuts[1:]:
        factor_of = factor_of * one(*cut)
    return factor_of


def setup_inputs(seed: int = 0) -> dict:
    key_of = jax.random.split(jax.random.key(seed), 9)
    return {
        "populations": draw_populations(jax.random.fold_in(key_of[8], 71), 0),
        "solid": touch_ends((jax.random.randint(key_of[1], (NX, NY, NZ), 0, 8) < 1).astype(jnp.int32), jax.random.fold_in(key_of[1], 1), 0, 1),
        "base_cell": draw_base_cell(jax.random.fold_in(key_of[8], 71), 0),
        "offset": jnp.clip(1.0 * jax.random.uniform(key_of[3], (3, N_GX, N_GY, MEMBRANE_SLOTS, PADDED_VERTICES), jnp.float32) ** block_levels(key_of[3], (3, N_GX, N_GY, MEMBRANE_SLOTS, PADDED_VERTICES), ((1, 4), (2, 8)), -0.2, 0.2), 0.0, 1.0),
        "rest_displacement": jnp.clip(1.0 * jax.random.uniform(key_of[4], (3, N_GX, N_GY, MEMBRANE_SLOTS, PADDED_VERTICES), jnp.float32) ** block_levels(key_of[4], (3, N_GX, N_GY, MEMBRANE_SLOTS, PADDED_VERTICES), ((1, 4), (2, 8)), -0.2, 0.2), 0.0, 1.0),
        "stiffness": jnp.clip(jnp.exp(math.log(0.063800626) - 2.3025852 * jax.random.uniform(key_of[5], (N_GX, N_GY, MEMBRANE_SLOTS), jnp.float32) ** block_levels(key_of[5], (N_GX, N_GY, MEMBRANE_SLOTS), ((0, 4), (1, 8)), -0.2, 0.2)), 0.006380062, 0.063800626),
        "occupied": draw_occupied(jax.random.fold_in(key_of[8], 71), 0),
        "triangles": draw_triangles(jax.random.fold_in(key_of[8], 71), 0),
    }


VELOCITIES = [[0, 0, 0], [1, 0, 0], [-1, 0, 0], [0, 1, 0], [0, -1, 0], [0, 0, 1], [0, 0, -1], [1, 1, 0], [-1, -1, 0], [1, -1, 0], [-1, 1, 0], [1, 0, 1], [-1, 0, -1], [1, 0, -1], [-1, 0, 1], [0, 1, 1], [0, -1, -1], [0, 1, -1], [0, -1, 1]]
OPPOSITE = [0, 2, 1, 4, 3, 6, 5, 8, 7, 10, 9, 12, 11, 14, 13, 16, 15, 18, 17]
LATTICE_WEIGHTS = [1.0 / 3.0] + [1.0 / 18.0] * 6 + [1.0 / 36.0] * 12
RELAX = 0.8


def kernel_weights(offset):
    return jnp.stack([(1.0 + jnp.cos(math.pi * (stencil_shift - offset) / 2.0)) / 4.0 for stencil_shift in (-1, 0, 1, 2)])


def membrane_force(offset, rest_displacement, stiffness, occupied, triangles):
    strain = offset - rest_displacement
    corners = [triangles[:, 0], triangles[:, 1], triangles[:, 2]]
    summed = strain[..., corners[0]] + strain[..., corners[1]] + strain[..., corners[2]]
    pulled_populations = jnp.zeros_like(strain)
    counts = jnp.zeros((strain.shape[-1],), jnp.float32)
    for corner in corners:
        pulled_populations = pulled_populations.at[..., corner].add(summed)
        counts = counts.at[corner].add(1.0)
    scaling = (stiffness * occupied.astype(jnp.float32))[None, :, :, :, None]
    return scaling * (pulled_populations - 3.0 * counts * strain)


def macro_state(populations, force_cell):
    density = jnp.sum(populations, axis=0)
    velocity_parts = []
    for dimension in range(3):
        moving = force_cell[dimension] * 0.5
        for lattice_direction in range(19):
            component = VELOCITIES[lattice_direction][dimension]
            if component != 0:
                moving = moving + component * populations[lattice_direction]
        velocity_parts.append(moving / density)
    return density, jnp.stack(velocity_parts)


def collide(populations, force_cell, solid):
    density, velocity = macro_state(populations, force_cell)
    squared = velocity[0] * velocity[0] + velocity[1] * velocity[1] + velocity[2] * velocity[2]
    working = velocity[0] * force_cell[0] + velocity[1] * force_cell[1] + velocity[2] * force_cell[2]
    walled = solid != 0
    relaxed = []
    for lattice_direction in range(19):
        vector = VELOCITIES[lattice_direction]
        along = vector[0] * velocity[0] + vector[1] * velocity[1] + vector[2] * velocity[2]
        pushed = vector[0] * force_cell[0] + vector[1] * force_cell[1] + vector[2] * force_cell[2]
        equilibrium = LATTICE_WEIGHTS[lattice_direction] * density * (1.0 + 3.0 * along + 4.5 * along * along - 1.5 * squared)
        source = (1.0 - 0.5 / RELAX) * LATTICE_WEIGHTS[lattice_direction] * (3.0 * (pushed - working) + 9.0 * along * pushed)
        current = populations[lattice_direction]
        updated = current - (current - equilibrium) / RELAX + source
        relaxed.append(jnp.where(walled, populations[OPPOSITE[lattice_direction]], updated))
    return relaxed


def reference(populations, solid, base_cell, offset, rest_displacement, stiffness, occupied, triangles):
    lattice = (NX, NY, NZ)
    cells = NX * NY * NZ
    coordinates = [[(base_cell[dimension] + stencil_shift) % lattice[dimension] for stencil_shift in (-1, 0, 1, 2)] for dimension in range(3)]
    live = occupied.astype(jnp.float32)[None, :, :, :, None]
    for substep in range(SUBSTEPS):
        force_vertex = membrane_force(offset, rest_displacement, stiffness, occupied, triangles)
        kernels = kernel_weights(offset)
        grid = jnp.zeros((3, cells), jnp.float32)
        for first in range(4):
            for second in range(4):
                for third in range(4):
                    index = (coordinates[0][first] * NY + coordinates[1][second]) * NZ + coordinates[2][third]
                    weight = kernels[first][0] * kernels[second][1] * kernels[third][2]
                    grid = grid.at[:, index.reshape(-1)].add((force_vertex * weight[None]).reshape(3, -1))
        force_cell = grid.reshape(3, NX, NY, NZ)
        relaxed = collide(populations, force_cell, solid)
        populations = jnp.stack([jnp.roll(relaxed[lattice_direction], tuple(VELOCITIES[lattice_direction]), axis=(0, 1, 2)) for lattice_direction in range(19)])
        flow = macro_state(populations, force_cell)[1].reshape(3, cells)
        moved = jnp.zeros_like(offset)
        for first in range(4):
            for second in range(4):
                for third in range(4):
                    index = (coordinates[0][first] * NY + coordinates[1][second]) * NZ + coordinates[2][third]
                    weight = kernels[first][0] * kernels[second][1] * kernels[third][2]
                    moved = moved + weight[None] * flow[:, index.reshape(-1)].reshape(offset.shape)
        offset = offset + live * moved
    return populations, offset
```

```python
import functools
import math

import jax
import jax.numpy as jnp
from jax import lax
from jax.experimental import pallas as pl
from jax.experimental.pallas import tpu as pltpu
from jax.sharding import PartitionSpec as P

SUBSTEPS = 3
VELOCITIES = [
    (0, 0, 0), (1, 0, 0), (-1, 0, 0), (0, 1, 0), (0, -1, 0), (0, 0, 1), (0, 0, -1),
    (1, 1, 0), (-1, -1, 0), (1, -1, 0), (-1, 1, 0), (1, 0, 1), (-1, 0, -1), (1, 0, -1),
    (-1, 0, 1), (0, 1, 1), (0, -1, -1), (0, 1, -1), (0, -1, 1),
]
OPPOSITE = [0, 2, 1, 4, 3, 6, 5, 8, 7, 10, 9, 12, 11, 14, 13, 16, 15, 18, 17]
LATTICE_WEIGHTS = [1.0 / 3.0] + [1.0 / 18.0] * 6 + [1.0 / 36.0] * 12
RELAX = 0.8
XS = {s: [q for q in range(19) if VELOCITIES[q][0] == s] for s in (1, -1)}
YS = {s: [q for q in range(19) if VELOCITIES[q][1] == s] for s in (1, -1)}
CORNER = {(v[0], v[1]): q for q, v in enumerate(VELOCITIES) if v[0] and v[1]}
DIRS = [(1, 0), (-1, 0), (0, 1), (0, -1), (1, 1), (1, -1), (-1, 1), (-1, -1)]
MESH = pl.DeviceIdType.MESH
NT = (((1,), (1,)), ((), ()))
NN = (((1,), (0,)), ((), ()))


def mm(a, b, dims):
    return lax.dot_general(a, b, dims, preferred_element_type=jnp.float32)


def split(value):
    high = value.astype(jnp.bfloat16)
    low = (value - high.astype(jnp.float32)).astype(jnp.bfloat16)
    return high, low


def quarter_sine(t):
    t = t - 4.0 * jnp.floor(t * 0.25 + 0.5)
    t = jnp.where(t > 1.0, 2.0 - t, jnp.where(t < -1.0, -2.0 - t, t))
    x = t * (math.pi / 2.0)
    u = x * x
    p = 1.0 / 6227020800.0
    for c in (-1.0 / 39916800.0, 1.0 / 362880.0, -1.0 / 5040.0, 1.0 / 120.0, -1.0 / 6.0, 1.0):
        p = p * u + c
    return x * p


def table(rows, base, kernels):
    cells = lax.broadcasted_iota(jnp.int32, (rows, base.shape[1]), 0)
    d = (cells - base + 1) & (rows - 1)
    out = jnp.where(d == 3, kernels[3], 0.0)
    for s in (2, 1, 0):
        out = jnp.where(d == s, kernels[s], out)
    return out


def moments(pops):
    density = functools.reduce(lambda a, b: a + b, pops)
    momentum = []
    for a in range(3):
        plus = [pops[q] for q in range(19) if VELOCITIES[q][a] == 1]
        minus = [pops[q] for q in range(19) if VELOCITIES[q][a] == -1]
        momentum.append(
            functools.reduce(lambda a, b: a + b, plus)
            - functools.reduce(lambda a, b: a + b, minus)
        )
    return density, momentum


def collide(pops, force, walled):
    density, momentum = moments(pops)
    inverse = 1.0 / density
    u = [(momentum[a] + 0.5 * force[a]) * inverse for a in range(3)]
    squared = u[0] * u[0] + u[1] * u[1] + u[2] * u[2]
    working = u[0] * force[0] + u[1] * force[1] + u[2] * force[2]
    base = 1.0 - 1.5 * squared
    relaxed = []
    for q in range(19):
        vector = VELOCITIES[q]
        along, pushed = jnp.zeros_like(density), jnp.zeros_like(density)
        for a in range(3):
            if vector[a] == 1:
                along, pushed = along + u[a], pushed + force[a]
            elif vector[a] == -1:
                along, pushed = along - u[a], pushed - force[a]
        w = LATTICE_WEIGHTS[q]
        equilibrium = (w * density) * (base + along * (3.0 + 4.5 * along))
        source = ((1.0 - 0.5 / RELAX) * w) * (3.0 * (pushed - working) + 9.0 * along * pushed)
        updated = pops[q] - (pops[q] - equilibrium) * (1.0 / RELAX) + source
        relaxed.append(jnp.where(walled, pops[OPPOSITE[q]], updated))
    return relaxed


def roll(x, shift, axis):
    size = x.shape[axis]
    shift = shift % size
    return x if shift == 0 else pltpu.roll(x, shift, axis)


def body_kernel(
    peers_x, peers_y,
    pops_ref, solid_ref, base_ref, offset_ref, rest_ref, stiff_ref, occ_ref, tri_ref,
    pops_out, offset_out,
    inc, lap, off, spread, grid, out_pops, out_flow, wide,
    *scratch,
):
    recv_force, recv_pops, recv_flow = scratch[0:8], scratch[8:16], scratch[16:24]
    send_px, send_py, send_pc = scratch[24:26], scratch[26:28], scratch[28:32]
    send_sem, recv_sem = scratch[32:34]
    rows_x = pops_ref.shape[1]
    depth = pops_ref.shape[3]
    slots, padded = base_ref.shape[1], base_ref.shape[2]
    vertices = slots * padded
    planes = rows_x + 3
    ix, iy = lax.axis_index("gx"), lax.axis_index("gy")
    peer = [((ix + sx + peers_x) % peers_x, (iy + sy + peers_y) % peers_y) for sx, sy in DIRS]

    barrier = pltpu.get_barrier_semaphore()
    for p in peer:
        pl.semaphore_signal(barrier, inc=1, device_id=p, device_id_type=MESH)

    ids = lax.broadcasted_iota(jnp.int32, inc.shape, 0)
    hit = (ids == tri_ref[0:1, :]) | (ids == tri_ref[1:2, :]) | (ids == tri_ref[2:3, :])
    inc[...] = jnp.where(hit, 1.0, 0.0).astype(jnp.bfloat16)
    pairs = mm(inc[...], inc[...], NT)
    same = lax.broadcasted_iota(jnp.int32, pairs.shape, 0) == lax.broadcasted_iota(
        jnp.int32, pairs.shape, 1
    )
    lap_high, lap_low = split(jnp.where(same, -2.0 * pairs, pairs))
    lap[0] = lap_high
    lap[1] = lap_low

    def flat(ref):
        return jnp.concatenate([ref[:, m, :] for m in range(slots)], axis=1)

    base = flat(base_ref)
    base_x = base[0:1] - ix * rows_x
    base_y = base[1:2] - iy * pops_ref.shape[2]
    base_z = base[2:3]
    live = jnp.concatenate(
        [jnp.full((1, padded), occ_ref[m].astype(jnp.float32)) for m in range(slots)], axis=1
    )
    scale = live * jnp.concatenate(
        [jnp.full((1, padded), stiff_ref[m]) for m in range(slots)], axis=1
    )
    off[...] = flat(offset_ref)
    pops_out[...] = pops_ref[...]
    sub = lax.broadcasted_iota(jnp.int32, (8, depth), 0)
    pl.semaphore_wait(barrier, len(peer))

    def copy(step, stage, d, src, dst):
        return pltpu.make_async_remote_copy(
            src_ref=src, dst_ref=dst.at[step], send_sem=send_sem.at[step, stage, d],
            recv_sem=recv_sem.at[step, stage, d], device_id=peer[d], device_id_type=MESH,
        )

    def force_copies(step):
        part = {1: pl.ds(rows_x, 2), -1: pl.ds(rows_x + 2, 1), 0: pl.ds(0, rows_x)}
        return [
            copy(step, 0, d, grid.at[step, part[sx], :, 0 if sy == 0 else 1], recv_force[d])
            for d, (sx, sy) in enumerate(DIRS)
        ]

    def pops_copies(step):
        src = list(send_px) + list(send_py) + list(send_pc)
        return [copy(step, 1, d, src[d].at[step], recv_pops[d]) for d in range(8)]

    def flow_copies(step):
        part = {1: pl.ds(rows_x - 1, 1), -1: pl.ds(0, 2), 0: pl.ds(0, rows_x)}
        return [
            copy(step, 2, d, out_flow.at[step, part[sx]], recv_flow[d])
            for d, (sx, sy) in enumerate(DIRS)
        ]

    def substep(step, carry):
        now = off[...]
        strain = now - flat(rest_ref)
        six = jnp.concatenate(
            [strain[:, m * padded : (m + 1) * padded] for m in range(slots)], axis=0
        )
        six_high = six.astype(jnp.bfloat16).astype(jnp.float32)
        both = jnp.concatenate([six_high, six - six_high], axis=0).astype(jnp.bfloat16)
        pulled = mm(both, lap[0], NN) + mm(both, lap[1], NN)
        pulled = pulled[0 : 3 * slots] + pulled[3 * slots :]
        force_v = scale * jnp.concatenate(
            [pulled[3 * m : 3 * m + 3] for m in range(slots)], axis=1
        )
        s = quarter_sine(now) * 0.25
        c = quarter_sine(now + 1.0) * 0.25
        kernels = (0.25 - s, 0.25 + c, 0.25 + s, 0.25 - c)
        table_x = table(8, base_x, [k[0:1] for k in kernels])
        table_y = table(16, base_y, [k[1:2] for k in kernels])
        deep_high, deep_low = split(table(depth, base_z, [k[2:3] for k in kernels]))
        deep = jnp.concatenate([deep_high, deep_low], axis=0)
        order = list(range(rows_x + 2)) + [7]
        for i, x in enumerate(order):
            for a in range(3):
                block = (force_v[a : a + 1] * table_x[x : x + 1]) * table_y
                high, low = split(block)
                row = (3 * i + a) * 16
                spread[0, row : row + 16, :] = high
                spread[1, row : row + 16, :] = low
        first = mm(spread[0], deep, NT)
        total = first[:, :depth] + first[:, depth:] + mm(spread[1], deep_high, NT)
        grid[step] = total.reshape(planes, 3, 2, 8, depth)
        sends = force_copies(step)
        for x in sends:
            x.start()
        for x in sends:
            x.wait_recv()
        R = {dv: recv_force[d][step] for d, dv in enumerate(DIRS)}
        low_rows = sub < 4
        total = grid[step, 0:rows_x, :, 0] + jnp.where(low_rows, R[0, 1], R[0, -1])
        left = R[1, 0] + jnp.where(low_rows, R[1, 1], R[1, -1])
        right = R[-1, 0] + jnp.where(low_rows, R[-1, 1], R[-1, -1])
        total = jnp.concatenate(
            [total[0:2] + left, total[2 : rows_x - 1], total[rows_x - 1 :] + right], axis=0
        )
        force = [total[:, a] for a in range(3)]

        relaxed = collide([pops_out[q] for q in range(19)], force, solid_ref[...] != 0)
        moved = [
            roll(roll(relaxed[q], VELOCITIES[q][2], 2), VELOCITIES[q][1], 1) for q in range(19)
        ]
        for n, sx in enumerate((1, -1)):
            edge = rows_x - 1 if sx == 1 else 0
            for k, q in enumerate(XS[sx]):
                send_px[n][step, k] = moved[q][edge]
        for n, sy in enumerate((1, -1)):
            packed = moved[YS[sy][0]]
            start = 0 if sy == 1 else 7
            for k, q in enumerate(YS[sy][1:], 1):
                packed = jnp.where(sub == (start + k) % 8, roll(moved[q], k, 1), packed)
            send_py[n][step] = packed
        for n, (sx, sy) in enumerate(DIRS[4:]):
            send_pc[n][step] = moved[CORNER[sx, sy]][rows_x - 1 if sx == 1 else 0]
        sends = pops_copies(step)
        for x in sends:
            x.start()
        for x in sends:
            x.wait_recv()
        from_y = {1: recv_pops[2][step], -1: recv_pops[3][step]}
        fresh = []
        for q in range(19):
            sx, sy, _ = VELOCITIES[q]
            value = moved[q]
            edge_row = sub == (0 if sy == 1 else 7)
            if sy:
                value = jnp.where(edge_row, roll(from_y[sy], -YS[sy].index(q), 1), value)
            if sx:
                side = recv_pops[0 if sx == 1 else 1][step, XS[sx].index(q)]
                if sy:
                    side = jnp.where(edge_row, recv_pops[DIRS.index((sx, sy))][step], side)
                if sx == 1:
                    value = jnp.concatenate([side[None], value[:-1]], axis=0)
                else:
                    value = jnp.concatenate([value[1:], side[None]], axis=0)
            pops_out[q] = value
            fresh.append(value)
        density, momentum = moments(fresh)
        inverse = 1.0 / density
        for a in range(3):
            out_flow[step, :, a] = (momentum[a] + 0.5 * force[a]) * inverse
        sends = flow_copies(step)
        for x in sends:
            x.start()
        for x in sends:
            x.wait_recv()
        R = {dv: recv_flow[d][step] for d, dv in enumerate(DIRS)}
        wide[0:rows_x, :, 0] = out_flow[step]
        wide[0:rows_x, :, 1] = jnp.where(low_rows, R[0, -1], R[0, 1])
        wide[rows_x : rows_x + 2, :, 0] = R[-1, 0]
        wide[rows_x : rows_x + 2, :, 1] = jnp.where(low_rows, R[-1, -1], R[-1, 1])
        wide[rows_x + 2 :, :, 0] = R[1, 0]
        wide[rows_x + 2 :, :, 1] = jnp.where(low_rows, R[1, -1], R[1, 1])
        wide_high, wide_low = split(wide[...].reshape(planes * 3 * 16, depth))
        twice = jnp.concatenate([wide_high, wide_high], axis=1)
        along = mm(twice, deep, NN) + mm(wide_low, deep_high, NN)
        along = along.reshape(planes, 3, 16, vertices)
        drift = []
        for a in range(3):
            acc = along[0, a] * table_x[0:1]
            for i, x in enumerate(order[1:], 1):
                acc = acc + along[i, a] * table_x[x : x + 1]
            drift.append(jnp.sum(acc * table_y, axis=0, keepdims=True))
        off[...] = now + live * jnp.concatenate(drift, axis=0)
        return carry

    lax.fori_loop(0, SUBSTEPS, substep, 0)

    for m in range(slots):
        offset_out[:, m, :] = off[:, m * padded : (m + 1) * padded]

    def drain(step, carry):
        for x in force_copies(step) + pops_copies(step) + flow_copies(step):
            x.wait_send()
        return carry

    lax.fori_loop(0, SUBSTEPS, drain, 0)


def local(mesh, populations, solid, base_cell, offset, rest, stiffness, occupied, triangles):
    rows_x, rows_y, depth = populations.shape[1:]
    slots, padded = offset.shape[3:]
    assert rows_y == 8 and 3 <= rows_x <= 5 and depth & (depth - 1) == 0
    vertices, planes, faces = slots * padded, rows_x + 3, triangles.shape[0]
    S = SUBSTEPS
    f32, bf16 = jnp.float32, jnp.bfloat16
    tile = (8, depth)
    n_force = {1: 2, -1: 1, 0: rows_x}
    n_flow = {1: 1, -1: 2, 0: rows_x}
    pop_shapes = [(5,)] * 2 + [(rows_x,)] * 2 + [()] * 4
    V = lambda shape, dtype=f32: pltpu.VMEM(shape, dtype)
    scratch = [
        V((padded, faces), bf16), V((2, padded, padded), bf16), V((3, vertices)),
        V((2, planes * 48, vertices), bf16), V((S, planes, 3, 2) + tile),
        V((8, depth)), V((S, rows_x, 3) + tile), V((planes, 3, 2) + tile),
    ]
    scratch += [V((S, n_force[sx], 3) + tile) for sx, sy in DIRS]
    scratch += [V((S,) + p + tile) for p in pop_shapes]
    scratch += [V((S, n_flow[sx], 3) + tile) for sx, sy in DIRS]
    scratch += [V((S,) + p + tile) for p in pop_shapes]
    scratch += [pltpu.SemaphoreType.DMA((S, 3, 8)), pltpu.SemaphoreType.DMA((S, 3, 8))]
    vmem = pl.BlockSpec(memory_space=pltpu.VMEM)
    smem = pl.BlockSpec(memory_space=pltpu.SMEM)
    small = (3, slots, padded)
    pops, moved = pl.pallas_call(
        functools.partial(body_kernel, mesh.shape["gx"], mesh.shape["gy"]),
        out_shape=(
            jax.ShapeDtypeStruct(populations.shape, f32),
            jax.ShapeDtypeStruct(small, f32),
        ),
        in_specs=[vmem] * 5 + [smem] * 2 + [vmem],
        out_specs=(vmem, vmem),
        scratch_shapes=scratch,
        compiler_params=pltpu.CompilerParams(
            collective_id=0, has_side_effects=True, vmem_limit_bytes=60 * 1024 * 1024
        ),
    )(
        populations, solid, base_cell.reshape(small), offset.reshape(small), rest.reshape(small),
        stiffness.reshape(slots), occupied.reshape(slots), triangles.T,
    )
    return pops, moved.reshape(offset.shape)


def solution(mesh):
    in_specs = (
        P(None, "gx", "gy", None),
        P("gx", "gy", None),
        P(None, "gx", "gy", None, None),
        P(None, "gx", "gy", None, None),
        P(None, "gx", "gy", None, None),
        P("gx", "gy", None),
        P("gx", "gy", None),
        P(),
    )
    out_specs = (P(None, "gx", "gy", None), P(None, "gx", "gy", None, None))
    return jax.shard_map(
        functools.partial(local, mesh), mesh=mesh, in_specs=in_specs, out_specs=out_specs,
        check_vma=False,
    )
```

```python
import functools
import math

import jax
import jax.numpy as jnp
from jax import lax
from jax.experimental import pallas as pl
from jax.experimental.pallas import tpu as pltpu
from jax.sharding import PartitionSpec as P

SUBSTEPS = 3
VELOCITIES = [
    (0, 0, 0), (1, 0, 0), (-1, 0, 0), (0, 1, 0), (0, -1, 0), (0, 0, 1), (0, 0, -1),
    (1, 1, 0), (-1, -1, 0), (1, -1, 0), (-1, 1, 0), (1, 0, 1), (-1, 0, -1), (1, 0, -1),
    (-1, 0, 1), (0, 1, 1), (0, -1, -1), (0, 1, -1), (0, -1, 1),
]
OPPOSITE = [0, 2, 1, 4, 3, 6, 5, 8, 7, 10, 9, 12, 11, 14, 13, 16, 15, 18, 17]
LATTICE_WEIGHTS = [1.0 / 3.0] + [1.0 / 18.0] * 6 + [1.0 / 36.0] * 12
RELAX = 0.8
XS = {s: [q for q in range(19) if VELOCITIES[q][0] == s] for s in (1, -1)}
YS = {s: [q for q in range(19) if VELOCITIES[q][1] == s] for s in (1, -1)}
CORNER = {(v[0], v[1]): q for q, v in enumerate(VELOCITIES) if v[0] and v[1]}
DIRS = [(1, 0), (-1, 0), (0, 1), (0, -1), (1, 1), (1, -1), (-1, 1), (-1, -1)]
MESH = pl.DeviceIdType.MESH
NT = (((1,), (1,)), ((), ()))
NN = (((1,), (0,)), ((), ()))


def mm(a, b, dims):
    return lax.dot_general(a, b, dims, preferred_element_type=jnp.float32)


def split(value):
    high = value.astype(jnp.bfloat16)
    low = (value - high.astype(jnp.float32)).astype(jnp.bfloat16)
    return high, low


def quarter_sine(t):
    t = t - 4.0 * jnp.floor(t * 0.25 + 0.5)
    t = jnp.where(t > 1.0, 2.0 - t, jnp.where(t < -1.0, -2.0 - t, t))
    x = t * (math.pi / 2.0)
    u = x * x
    p = 1.0 / 6227020800.0
    for c in (-1.0 / 39916800.0, 1.0 / 362880.0, -1.0 / 5040.0, 1.0 / 120.0, -1.0 / 6.0, 1.0):
        p = p * u + c
    return x * p


def table(rows, base, kernels):
    cells = lax.broadcasted_iota(jnp.int32, (rows, base.shape[1]), 0)
    d = (cells - base + 1) & (rows - 1)
    out = jnp.where(d == 3, kernels[3], 0.0)
    for s in (2, 1, 0):
        out = jnp.where(d == s, kernels[s], out)
    return out


def moments(pops):
    density = functools.reduce(lambda a, b: a + b, pops)
    momentum = []
    for a in range(3):
        plus = [pops[q] for q in range(19) if VELOCITIES[q][a] == 1]
        minus = [pops[q] for q in range(19) if VELOCITIES[q][a] == -1]
        momentum.append(
            functools.reduce(lambda a, b: a + b, plus)
            - functools.reduce(lambda a, b: a + b, minus)
        )
    return density, momentum


def collide(pops, force, walled):
    density, momentum = moments(pops)
    inverse = 1.0 / density
    u = [(momentum[a] + 0.5 * force[a]) * inverse for a in range(3)]
    squared = u[0] * u[0] + u[1] * u[1] + u[2] * u[2]
    working = u[0] * force[0] + u[1] * force[1] + u[2] * force[2]
    base = 1.0 - 1.5 * squared
    relaxed = []
    for q in range(19):
        vector = VELOCITIES[q]
        along, pushed = jnp.zeros_like(density), jnp.zeros_like(density)
        for a in range(3):
            if vector[a] == 1:
                along, pushed = along + u[a], pushed + force[a]
            elif vector[a] == -1:
                along, pushed = along - u[a], pushed - force[a]
        w = LATTICE_WEIGHTS[q]
        equilibrium = (w * density) * (base + along * (3.0 + 4.5 * along))
        source = ((1.0 - 0.5 / RELAX) * w) * (3.0 * (pushed - working) + 9.0 * along * pushed)
        updated = pops[q] - (pops[q] - equilibrium) * (1.0 / RELAX) + source
        relaxed.append(jnp.where(walled, pops[OPPOSITE[q]], updated))
    return relaxed


def roll(x, shift, axis):
    size = x.shape[axis]
    shift = shift % size
    return x if shift == 0 else pltpu.roll(x, shift, axis)


def row_mask(start, rows, depth):
    sub = lax.broadcasted_iota(jnp.int32, (8, depth), 0)
    return ((sub - start) & 7) < rows


def pack(tiles, start, rows):
    per, out = 8 // rows, []
    for g in range(0, len(tiles), per):
        acc = tiles[g]
        for k, tile in enumerate(tiles[g + 1 : g + per], 1):
            mask = row_mask(start + k * rows, rows, tile.shape[1])
            acc = jnp.where(mask, roll(tile, k * rows, 0), acc)
        out.append(acc)
    return out


def unpack(load, count, rows):
    per = 8 // rows
    return [roll(load(k // per), -(k % per) * rows, 0) for k in range(count)]


def packed(count, rows):
    return -(-count // (8 // rows))


def force_planes(sx, rows_x):
    return {1: [rows_x, rows_x + 1], -1: [-1], 0: list(range(rows_x))}[sx]


def moment_planes(sx, rows_x):
    return {1: [rows_x - 1, rows_x], -1: [-1, 0, 1], 0: list(range(-1, rows_x + 1))}[sx]


def landing(x, sx, rows_x):
    return x - sx * rows_x


def force_size(sx, sy, rows_x):
    n = 3 * len(force_planes(sx, rows_x))
    return {0: n, 1: packed(n, 2), -1: packed(n, 1)}[sy]


def moment_size(sx, sy, rows_x):
    n = 4 * len(moment_planes(sx, rows_x))
    return {0: n + packed(n, 2), 1: packed(n, 2), -1: packed(n, 1) + packed(n, 2)}[sy]


def total_of(parts):
    return functools.reduce(lambda a, b: a + b, parts)


def body_kernel(
    peers_x, peers_y,
    pops_ref, solid_ref, base_ref, offset_ref, rest_ref, stiff_ref, occ_ref, tri_ref,
    pops_out, offset_out,
    inc, lap, off, spread, moved_ref, wide,
    *scratch,
):
    recv_force, recv_pops, recv_mom = scratch[0:8], scratch[8:16], scratch[16:24]
    send_force, send_pops, send_mom = scratch[24:32], scratch[32:40], scratch[40:48]
    send_px, send_py, send_pc = send_pops[0:2], send_pops[2:4], send_pops[4:8]
    send_sem, recv_sem = scratch[48:50]
    rows_x = pops_ref.shape[1]
    depth = pops_ref.shape[3]
    slots, padded = base_ref.shape[1], base_ref.shape[2]
    vertices = slots * padded
    planes = rows_x + 3
    ix, iy = lax.axis_index("gx"), lax.axis_index("gy")
    peer = [((ix + sx + peers_x) % peers_x, (iy + sy + peers_y) % peers_y) for sx, sy in DIRS]

    barrier = pltpu.get_barrier_semaphore()
    for p in peer:
        pl.semaphore_signal(barrier, inc=1, device_id=p, device_id_type=MESH)

    ids = lax.broadcasted_iota(jnp.int32, inc.shape, 0)
    hit = (ids == tri_ref[0:1, :]) | (ids == tri_ref[1:2, :]) | (ids == tri_ref[2:3, :])
    inc[...] = jnp.where(hit, 1.0, 0.0).astype(jnp.bfloat16)
    pairs = mm(inc[...], inc[...], NT)
    same = lax.broadcasted_iota(jnp.int32, pairs.shape, 0) == lax.broadcasted_iota(
        jnp.int32, pairs.shape, 1
    )
    lap_high, lap_low = split(jnp.where(same, -2.0 * pairs, pairs))
    lap[0] = lap_high
    lap[1] = lap_low

    def flat(ref):
        return jnp.concatenate([ref[:, m, :] for m in range(slots)], axis=1)

    base = flat(base_ref)
    base_x = base[0:1] - ix * rows_x
    base_y = base[1:2] - iy * pops_ref.shape[2]
    base_z = base[2:3]
    live = jnp.concatenate(
        [jnp.full((1, padded), occ_ref[m].astype(jnp.float32)) for m in range(slots)], axis=1
    )
    scale = live * jnp.concatenate(
        [jnp.full((1, padded), stiff_ref[m]) for m in range(slots)], axis=1
    )
    off[...] = flat(offset_ref)
    pops_out[...] = pops_ref[...]
    sub = lax.broadcasted_iota(jnp.int32, (8, depth), 0)
    pl.semaphore_wait(barrier, len(peer))

    def copy(step, stage, d, src, dst):
        return pltpu.make_async_remote_copy(
            src_ref=src, dst_ref=dst.at[step], send_sem=send_sem.at[step, stage, d],
            recv_sem=recv_sem.at[step, stage, d], device_id=peer[d], device_id_type=MESH,
        )

    groups = ((send_force, recv_force), (send_mom, recv_mom), (send_pops, recv_pops))

    def copies(step, stage):
        src, dst = groups[stage]
        return [copy(step, stage, d, src[d].at[step], dst[d]) for d in (4, 5, 6, 7, 2, 3, 0, 1)]

    def launch(step, stage):
        for x in copies(step, stage):
            x.start()

    def arrive(step, stage):
        for x in copies(step, stage):
            x.wait_recv()

    def finish_pops(step):
        arrive(step, 2)
        from_y = {1: recv_pops[2][step], -1: recv_pops[3][step]}
        for q in range(19):
            sx, sy, _ = VELOCITIES[q]
            value = moved_ref[q]
            edge_row = sub == (0 if sy == 1 else 7)
            if sy:
                value = jnp.where(edge_row, roll(from_y[sy], -YS[sy].index(q), 1), value)
            if sx:
                side = recv_pops[0 if sx == 1 else 1][step, XS[sx].index(q)]
                if sy:
                    side = jnp.where(edge_row, recv_pops[DIRS.index((sx, sy))][step], side)
                if sx == 1:
                    value = jnp.concatenate([side[None], value[:-1]], axis=0)
                else:
                    value = jnp.concatenate([value[1:], side[None]], axis=0)
            pops_out[q] = value

    def substep(step, carry):
        now = off[...]
        strain = now - flat(rest_ref)
        six = jnp.concatenate(
            [strain[:, m * padded : (m + 1) * padded] for m in range(slots)], axis=0
        )
        six_high = six.astype(jnp.bfloat16).astype(jnp.float32)
        both = jnp.concatenate([six_high, six - six_high], axis=0).astype(jnp.bfloat16)
        pulled = mm(both, lap[0], NN) + mm(both, lap[1], NN)
        pulled = pulled[0 : 3 * slots] + pulled[3 * slots :]
        force_v = scale * jnp.concatenate(
            [pulled[3 * m : 3 * m + 3] for m in range(slots)], axis=1
        )
        s = quarter_sine(now) * 0.25
        c = quarter_sine(now + 1.0) * 0.25
        kernels = (0.25 - s, 0.25 + c, 0.25 + s, 0.25 - c)
        table_x = table(8, base_x, [k[0:1] for k in kernels])
        table_y = table(16, base_y, [k[1:2] for k in kernels])
        deep_high, deep_low = split(table(depth, base_z, [k[2:3] for k in kernels]))
        deep = jnp.concatenate([deep_high, deep_low], axis=0)
        order = list(range(rows_x + 2)) + [7]
        for i, x in enumerate(order):
            for a in range(3):
                block = (force_v[a : a + 1] * table_x[x : x + 1]) * table_y
                high, low = split(block)
                row = (3 * i + a) * 16
                spread[0, row : row + 16, :] = high
                spread[1, row : row + 16, :] = low
        first = mm(spread[0], deep, NT)
        total = first[:, :depth] + first[:, depth:] + mm(spread[1], deep_high, NT)
        place = {x % (rows_x + 3): i for i, x in enumerate(list(range(rows_x + 2)) + [-1])}

        def tile_of(x, a, t):
            row = (3 * place[x % (rows_x + 3)] + a) * 16 + 8 * t
            return total[row : row + 8]

        for d, (sx, sy) in enumerate(DIRS):
            tiles = [
                tile_of(x, a, 0 if sy == 0 else 1)
                for x in force_planes(sx, rows_x) for a in range(3)
            ]
            if sy:
                tiles = pack(tiles, 0 if sy == 1 else 7, 2 if sy == 1 else 1)
            for k, tile in enumerate(tiles):
                send_force[d][step, k] = tile
        launch(step, 0)

        @pl.when(step > 0)
        def _():
            finish_pops(step - 1)

        arrive(step, 0)
        parts = {(x, a): [tile_of(x, a, 0)] for x in range(rows_x) for a in range(3)}
        for d, (sx, sy) in enumerate(DIRS):
            names = [
                (landing(x, sx, rows_x), a) for x in force_planes(sx, rows_x) for a in range(3)
            ]
            load = lambda k, d=d: recv_force[d][step, k]
            if sy == 0:
                tiles = [load(k) for k in range(len(names))]
            else:
                start, rows = (0, 2) if sy == 1 else (7, 1)
                mask = row_mask(start, rows, depth)
                tiles = [jnp.where(mask, t, 0.0) for t in unpack(load, len(names), rows)]
            for name, tile in zip(names, tiles):
                parts[name].append(tile)
        force = [
            jnp.stack([total_of(parts[x, a]) for x in range(rows_x)]) for a in range(3)
        ]

        relaxed = collide([pops_out[q] for q in range(19)], force, solid_ref[...] != 0)
        moved = [
            roll(roll(relaxed[q], VELOCITIES[q][2], 2), VELOCITIES[q][1], 1) for q in range(19)
        ]
        for q in range(19):
            moved_ref[q] = moved[q]
        nothing = jnp.zeros((1, 8, depth), jnp.float32)
        rho, mz = {}, {}
        for cx in (-1, 0, 1):
            for cy in (-1, 0, 1):
                members = [q for q in range(19) if VELOCITIES[q][:2] == (cx, cy)]
                pad = lambda v: jnp.concatenate(
                    [nothing] * (1 + cx) + [v] + [nothing] * (1 - cx), axis=0
                )
                rho[cx, cy] = pad(total_of([moved[q] for q in members]))
                up = [moved[q] for q in members if VELOCITIES[q][2] == 1]
                down = [moved[q] for q in members if VELOCITIES[q][2] == -1]
                if up:
                    mz[cx, cy] = pad(total_of(up) - total_of(down))
        first_row, last_row = sub == 0, sub == 7
        own = {}
        zero = jnp.zeros((rows_x + 2, 8, depth), jnp.float32)
        fields = []
        for cy in (0, 1, -1):
            dens = rho[-1, cy] + rho[0, cy] + rho[1, cy]
            deep_m = [mz[cx, cy] for cx in (-1, 0, 1) if (cx, cy) in mz]
            fields.append((
                dens, rho[1, cy] - rho[-1, cy], zero if cy == 0 else cy * dens, total_of(deep_m)
            ))
        for c in range(4):
            mid, up, down = (fields[g][c] for g in range(3))
            near = mid + jnp.where(first_row, 0.0, up) + jnp.where(last_row, 0.0, down)
            if c:
                half = 0.5 * force[c - 1]
                near = near + jnp.concatenate([nothing, half, nothing], axis=0)
            far = jnp.where(first_row, up, jnp.where(last_row, down, 0.0))
            for x in range(-1, rows_x + 1):
                own[x, c] = (near[x + 1], far[x + 1])
        for d, (sx, sy) in enumerate(DIRS):
            names = [(x, c) for x in moment_planes(sx, rows_x) for c in range(4)]
            near, far = [own[n][0] for n in names], [own[n][1] for n in names]
            if sy == 0:
                tiles = near + pack(far, 7, 2)
            elif sy == 1:
                tiles = pack([jnp.where(last_row, a, b) for a, b in zip(near, far)], 7, 2)
            else:
                tiles = pack(far, 7, 1) + pack(near, 0, 2)
            for k, tile in enumerate(tiles):
                send_mom[d][step, k] = tile
        launch(step, 1)
        for n, sx in enumerate((1, -1)):
            edge = rows_x - 1 if sx == 1 else 0
            for k, q in enumerate(XS[sx]):
                send_px[n][step, k] = moved[q][edge]
        for n, sy in enumerate((1, -1)):
            rows_kept = moved[YS[sy][0]]
            start = 0 if sy == 1 else 7
            for k, q in enumerate(YS[sy][1:], 1):
                rows_kept = jnp.where(sub == (start + k) % 8, roll(moved[q], k, 1), rows_kept)
            send_py[n][step] = rows_kept
        for n, (sx, sy) in enumerate(DIRS[4:]):
            send_pc[n][step] = moved[CORNER[sx, sy]][rows_x - 1 if sx == 1 else 0]
        launch(step, 2)
        arrive(step, 1)
        reach = [x for x in range(rows_x + 2)] + [-1]
        near = {(x, c): [] for x in reach for c in range(4)}
        far = {(x, c): [] for x in reach for c in range(4)}
        for name, (a, b) in own.items():
            near[name].append(a)
            far[name].append(b)
        two, edges, one = row_mask(0, 2, depth), row_mask(7, 2, depth), row_mask(7, 1, depth)
        for d, (sx, sy) in enumerate(DIRS):
            names = [
                (landing(x, sx, rows_x), c)
                for x in moment_planes(sx, rows_x) for c in range(4)
            ]
            count = len(names)
            load = lambda k, d=d: recv_mom[d][step, k]
            if sy == 0:
                a = [load(k) for k in range(count)]
                b = unpack(lambda k: load(count + k), count, 2)
                b = [jnp.where(edges, t, 0.0) for t in b]
            elif sy == 1:
                both_rows = unpack(load, count, 2)
                a = [jnp.where(first_row, t, 0.0) for t in both_rows]
                b = [jnp.where(last_row, t, 0.0) for t in both_rows]
            else:
                skip = packed(count, 1)
                a = [jnp.where(one, t, 0.0) for t in unpack(load, count, 1)]
                b = unpack(lambda k: load(skip + k), count, 2)
                b = [jnp.where(two, t, 0.0) for t in b]
            for name, p, r in zip(names, a, b):
                near[name].append(p)
                far[name].append(r)
        used = row_mask(7, 3, depth)
        for i, x in enumerate(reach):
            for t, side in enumerate((near, far)):
                dens = total_of(side[x, 0])
                if t:
                    dens = jnp.where(used, dens, 1.0)
                inverse = 1.0 / dens
                for a in range(3):
                    wide[i, a, t] = total_of(side[x, a + 1]) * inverse
        wide_high, wide_low = split(wide[...].reshape(planes * 3 * 16, depth))
        twice = jnp.concatenate([wide_high, wide_high], axis=1)
        along = mm(twice, deep, NN) + mm(wide_low, deep_high, NN)
        along = along.reshape(planes, 3, 16, vertices)
        drift, order = [], list(range(rows_x + 2)) + [7]
        for a in range(3):
            acc = along[0, a] * table_x[0:1]
            for i, x in enumerate(order[1:], 1):
                acc = acc + along[i, a] * table_x[x : x + 1]
            drift.append(jnp.sum(acc * table_y, axis=0, keepdims=True))
        off[...] = now + live * jnp.concatenate(drift, axis=0)
        return carry

    lax.fori_loop(0, SUBSTEPS, substep, 0)
    finish_pops(SUBSTEPS - 1)

    for m in range(slots):
        offset_out[:, m, :] = off[:, m * padded : (m + 1) * padded]

    def drain(step, carry):
        for stage in range(3):
            for x in copies(step, stage):
                x.wait_send()
        return carry

    lax.fori_loop(0, SUBSTEPS, drain, 0)


def local(mesh, populations, solid, base_cell, offset, rest, stiffness, occupied, triangles):
    rows_x, rows_y, depth = populations.shape[1:]
    slots, padded = offset.shape[3:]
    assert rows_y == 8 and 3 <= rows_x <= 5 and depth & (depth - 1) == 0
    vertices, planes, faces = slots * padded, rows_x + 3, triangles.shape[0]
    S = SUBSTEPS
    f32, bf16 = jnp.float32, jnp.bfloat16
    tile = (8, depth)
    pop_shapes = [(5,)] * 2 + [(rows_x,)] * 2 + [()] * 4
    V = lambda shape, dtype=f32: pltpu.VMEM(shape, dtype)
    scratch = [
        V((padded, faces), bf16), V((2, padded, padded), bf16), V((3, vertices)),
        V((2, planes * 48, vertices), bf16),
        V((19, rows_x) + tile), V((planes, 3, 2) + tile),
    ]
    for _ in ("receive", "send"):
        scratch += [V((S, force_size(*d, rows_x)) + tile) for d in DIRS]
        scratch += [V((S,) + p + tile) for p in pop_shapes]
        scratch += [V((S, moment_size(*d, rows_x)) + tile) for d in DIRS]
    scratch += [pltpu.SemaphoreType.DMA((S, 3, 8)), pltpu.SemaphoreType.DMA((S, 3, 8))]
    vmem = pl.BlockSpec(memory_space=pltpu.VMEM)
    smem = pl.BlockSpec(memory_space=pltpu.SMEM)
    small = (3, slots, padded)
    pops, moved = pl.pallas_call(
        functools.partial(body_kernel, mesh.shape["gx"], mesh.shape["gy"]),
        out_shape=(
            jax.ShapeDtypeStruct(populations.shape, f32),
            jax.ShapeDtypeStruct(small, f32),
        ),
        in_specs=[vmem] * 5 + [smem] * 2 + [vmem],
        out_specs=(vmem, vmem),
        scratch_shapes=scratch,
        compiler_params=pltpu.CompilerParams(
            collective_id=0, has_side_effects=True, vmem_limit_bytes=60 * 1024 * 1024
        ),
    )(
        populations, solid, base_cell.reshape(small), offset.reshape(small), rest.reshape(small),
        stiffness.reshape(slots), occupied.reshape(slots), triangles.T,
    )
    return pops, moved.reshape(offset.shape)


def solution(mesh):
    in_specs = (
        P(None, "gx", "gy", None),
        P("gx", "gy", None),
        P(None, "gx", "gy", None, None),
        P(None, "gx", "gy", None, None),
        P(None, "gx", "gy", None, None),
        P("gx", "gy", None),
        P("gx", "gy", None),
        P(),
    )
    out_specs = (P(None, "gx", "gy", None), P(None, "gx", "gy", None, None))
    return jax.shard_map(
        functools.partial(local, mesh), mesh=mesh, in_specs=in_specs, out_specs=out_specs,
        check_vma=False,
    )
```

```python
import functools
import math

import jax
import jax.numpy as jnp
from jax import lax
from jax.experimental import pallas as pl
from jax.experimental.pallas import tpu as pltpu
from jax.sharding import PartitionSpec as P

SUBSTEPS = 3
VELOCITIES = [
    (0, 0, 0), (1, 0, 0), (-1, 0, 0), (0, 1, 0), (0, -1, 0), (0, 0, 1), (0, 0, -1),
    (1, 1, 0), (-1, -1, 0), (1, -1, 0), (-1, 1, 0), (1, 0, 1), (-1, 0, -1), (1, 0, -1),
    (-1, 0, 1), (0, 1, 1), (0, -1, -1), (0, 1, -1), (0, -1, 1),
]
OPPOSITE = [0, 2, 1, 4, 3, 6, 5, 8, 7, 10, 9, 12, 11, 14, 13, 16, 15, 18, 17]
LATTICE_WEIGHTS = [1.0 / 3.0] + [1.0 / 18.0] * 6 + [1.0 / 36.0] * 12
RELAX = 0.8
XS = {s: [q for q in range(19) if VELOCITIES[q][0] == s] for s in (1, -1)}
YS = {s: [q for q in range(19) if VELOCITIES[q][1] == s] for s in (1, -1)}
CORNER = {(v[0], v[1]): q for q, v in enumerate(VELOCITIES) if v[0] and v[1]}
DIRS = [(1, 0), (-1, 0), (0, 1), (0, -1), (1, 1), (1, -1), (-1, 1), (-1, -1)]
MESH = pl.DeviceIdType.MESH
NT = (((1,), (1,)), ((), ()))
NN = (((1,), (0,)), ((), ()))


def mm(a, b, dims):
    return lax.dot_general(a, b, dims, preferred_element_type=jnp.float32)


def split(value):
    high = value.astype(jnp.bfloat16)
    low = (value - high.astype(jnp.float32)).astype(jnp.bfloat16)
    return high, low


def quarter_sine(t):
    t = t - 4.0 * jnp.floor(t * 0.25 + 0.5)
    t = jnp.where(t > 1.0, 2.0 - t, jnp.where(t < -1.0, -2.0 - t, t))
    x = t * (math.pi / 2.0)
    u = x * x
    p = 1.0 / 6227020800.0
    for c in (-1.0 / 39916800.0, 1.0 / 362880.0, -1.0 / 5040.0, 1.0 / 120.0, -1.0 / 6.0, 1.0):
        p = p * u + c
    return x * p


def table(rows, base, kernels):
    cells = lax.broadcasted_iota(jnp.int32, (rows, base.shape[1]), 0)
    d = (cells - base + 1) & (rows - 1)
    out = jnp.where(d == 3, kernels[3], 0.0)
    for s in (2, 1, 0):
        out = jnp.where(d == s, kernels[s], out)
    return out


def moments(pops):
    density = functools.reduce(lambda a, b: a + b, pops)
    momentum = []
    for a in range(3):
        plus = [pops[q] for q in range(19) if VELOCITIES[q][a] == 1]
        minus = [pops[q] for q in range(19) if VELOCITIES[q][a] == -1]
        momentum.append(
            functools.reduce(lambda a, b: a + b, plus)
            - functools.reduce(lambda a, b: a + b, minus)
        )
    return density, momentum


def collide(pops, force, walled):
    density, momentum = moments(pops)
    inverse = 1.0 / density
    u = [(momentum[a] + 0.5 * force[a]) * inverse for a in range(3)]
    squared = u[0] * u[0] + u[1] * u[1] + u[2] * u[2]
    working = u[0] * force[0] + u[1] * force[1] + u[2] * force[2]
    base = 1.0 - 1.5 * squared
    relaxed = []
    for q in range(19):
        vector = VELOCITIES[q]
        along, pushed = jnp.zeros_like(density), jnp.zeros_like(density)
        for a in range(3):
            if vector[a] == 1:
                along, pushed = along + u[a], pushed + force[a]
            elif vector[a] == -1:
                along, pushed = along - u[a], pushed - force[a]
        w = LATTICE_WEIGHTS[q]
        equilibrium = (w * density) * (base + along * (3.0 + 4.5 * along))
        source = ((1.0 - 0.5 / RELAX) * w) * (3.0 * (pushed - working) + 9.0 * along * pushed)
        updated = pops[q] - (pops[q] - equilibrium) * (1.0 / RELAX) + source
        relaxed.append(jnp.where(walled, pops[OPPOSITE[q]], updated))
    return relaxed


def roll(x, shift, axis):
    size = x.shape[axis]
    shift = shift % size
    return x if shift == 0 else pltpu.roll(x, shift, axis)


def row_mask(start, rows, depth):
    sub = lax.broadcasted_iota(jnp.int32, (8, depth), 0)
    return ((sub - start) & 7) < rows


def pack(tiles, start, rows):
    per, out = 8 // rows, []
    for g in range(0, len(tiles), per):
        acc = tiles[g]
        for k, tile in enumerate(tiles[g + 1 : g + per], 1):
            mask = row_mask(start + k * rows, rows, tile.shape[1])
            acc = jnp.where(mask, roll(tile, k * rows, 0), acc)
        out.append(acc)
    return out


def unpack(load, count, rows):
    per = 8 // rows
    return [roll(load(k // per), -(k % per) * rows, 0) for k in range(count)]


def packed(count, rows):
    return -(-count // (8 // rows))


def force_planes(sx, rows_x):
    return {1: [rows_x, rows_x + 1], -1: [-1], 0: list(range(rows_x))}[sx]


def moment_planes(sx, rows_x):
    return {1: [rows_x - 1, rows_x], -1: [-1, 0, 1], 0: list(range(-1, rows_x + 1))}[sx]


def landing(x, sx, rows_x):
    return x - sx * rows_x


def force_size(sx, sy, rows_x):
    n = 3 * len(force_planes(sx, rows_x))
    return {0: n, 1: packed(n, 2), -1: packed(n, 1)}[sy]


def moment_size(sx, sy, rows_x):
    n = 4 * len(moment_planes(sx, rows_x))
    return {0: n + packed(n, 2), 1: packed(n, 2), -1: packed(n, 1) + packed(n, 2)}[sy]


def total_of(parts):
    return functools.reduce(lambda a, b: a + b, parts)


def body_kernel(
    peers_x, peers_y,
    pops_ref, solid_ref, base_ref, offset_ref, rest_ref, stiff_ref, occ_ref, tri_ref,
    pops_out, offset_out,
    inc, lap, off, spread, moved_ref, wide,
    *scratch,
):
    recv_force, recv_pops, recv_mom = scratch[0:8], scratch[8:16], scratch[16:24]
    send_force, send_pops, send_mom = scratch[24:32], scratch[32:40], scratch[40:48]
    send_px, send_py, send_pc = send_pops[0:2], send_pops[2:4], send_pops[4:8]
    send_sem, recv_sem, load_sem = scratch[48:51]
    rows_x = pops_ref.shape[1]
    depth = pops_ref.shape[3]
    slots, padded = base_ref.shape[1], base_ref.shape[2]
    vertices = slots * padded
    planes = rows_x + 3
    ix, iy = lax.axis_index("gx"), lax.axis_index("gy")
    peer = [((ix + sx + peers_x) % peers_x, (iy + sy + peers_y) % peers_y) for sx, sy in DIRS]

    load_pops = pltpu.make_async_copy(pops_ref, pops_out, load_sem)
    load_pops.start()
    barrier = pltpu.get_barrier_semaphore()
    for p in peer:
        pl.semaphore_signal(barrier, inc=1, device_id=p, device_id_type=MESH)

    ids = lax.broadcasted_iota(jnp.int32, inc.shape, 0)
    hit = (ids == tri_ref[0:1, :]) | (ids == tri_ref[1:2, :]) | (ids == tri_ref[2:3, :])
    inc[...] = jnp.where(hit, 1.0, 0.0).astype(jnp.bfloat16)
    pairs = mm(inc[...], inc[...], NT)
    same = lax.broadcasted_iota(jnp.int32, pairs.shape, 0) == lax.broadcasted_iota(
        jnp.int32, pairs.shape, 1
    )
    lap_high, lap_low = split(jnp.where(same, -2.0 * pairs, pairs))
    lap[0] = lap_high
    lap[1] = lap_low

    def flat(ref):
        return jnp.concatenate([ref[:, m, :] for m in range(slots)], axis=1)

    base = flat(base_ref)
    base_x = base[0:1] - ix * rows_x
    base_y = base[1:2] - iy * pops_ref.shape[2]
    base_z = base[2:3]
    live = jnp.concatenate(
        [jnp.full((1, padded), occ_ref[m].astype(jnp.float32)) for m in range(slots)], axis=1
    )
    scale = live * jnp.concatenate(
        [jnp.full((1, padded), stiff_ref[m]) for m in range(slots)], axis=1
    )
    off[...] = flat(offset_ref)
    sub = lax.broadcasted_iota(jnp.int32, (8, depth), 0)
    load_pops.wait()
    pl.semaphore_wait(barrier, len(peer))

    def copy(step, stage, d, src, dst):
        return pltpu.make_async_remote_copy(
            src_ref=src, dst_ref=dst.at[step], send_sem=send_sem.at[step, stage, d],
            recv_sem=recv_sem.at[step, stage, d], device_id=peer[d], device_id_type=MESH,
        )

    groups = ((send_force, recv_force), (send_mom, recv_mom), (send_pops, recv_pops))

    def copies(step, stage):
        src, dst = groups[stage]
        return [copy(step, stage, d, src[d].at[step], dst[d]) for d in range(8)]

    def launch(step, stage):
        sends = copies(step, stage)

        @pl.when(iy % 2 == 1)
        def _():
            for d in (4, 6, 2, 5, 7, 3, 0, 1):
                sends[d].start()

        @pl.when(iy % 2 == 0)
        def _():
            for d in (5, 7, 3, 4, 6, 2, 0, 1):
                sends[d].start()

    def arrive(step, stage):
        for x in copies(step, stage):
            x.wait_recv()

    def finish_pops(step):
        arrive(step, 2)
        from_y = {1: recv_pops[2][step], -1: recv_pops[3][step]}
        for q in range(19):
            sx, sy, _ = VELOCITIES[q]
            value = moved_ref[q]
            edge_row = sub == (0 if sy == 1 else 7)
            if sy:
                value = jnp.where(edge_row, roll(from_y[sy], -YS[sy].index(q), 1), value)
            if sx:
                side = recv_pops[0 if sx == 1 else 1][step, XS[sx].index(q)]
                if sy:
                    side = jnp.where(edge_row, recv_pops[DIRS.index((sx, sy))][step], side)
                if sx == 1:
                    value = jnp.concatenate([side[None], value[:-1]], axis=0)
                else:
                    value = jnp.concatenate([value[1:], side[None]], axis=0)
            pops_out[q] = value

    def substep(step, carry):
        now = off[...]
        strain = now - flat(rest_ref)
        six = jnp.concatenate(
            [strain[:, m * padded : (m + 1) * padded] for m in range(slots)], axis=0
        )
        six_high = six.astype(jnp.bfloat16).astype(jnp.float32)
        both = jnp.concatenate([six_high, six - six_high], axis=0).astype(jnp.bfloat16)
        pulled = mm(both, lap[0], NN) + mm(both, lap[1], NN)
        pulled = pulled[0 : 3 * slots] + pulled[3 * slots :]
        force_v = scale * jnp.concatenate(
            [pulled[3 * m : 3 * m + 3] for m in range(slots)], axis=1
        )
        s = quarter_sine(now) * 0.25
        c = quarter_sine(now + 1.0) * 0.25
        kernels = (0.25 - s, 0.25 + c, 0.25 + s, 0.25 - c)
        table_x = table(8, base_x, [k[0:1] for k in kernels])
        table_y = table(16, base_y, [k[1:2] for k in kernels])
        deep_high, deep_low = split(table(depth, base_z, [k[2:3] for k in kernels]))
        deep = jnp.concatenate([deep_high, deep_low], axis=0)
        tiles_of = {}

        def spread_tiles(names, start):
            for n in range(0, len(names), 2):
                blocks = [
                    (force_v[a : a + 1] * table_x[x & 7 : (x & 7) + 1])
                    * table_y[8 * t : 8 * t + 8]
                    for x, a, t in names[n : n + 2]
                ]
                high, low = split(jnp.concatenate(blocks, axis=0))
                row = start + 8 * n
                spread[0, row : row + 16, :] = high
                spread[1, row : row + 16, :] = low
            stop = start + 8 * len(names)
            first = mm(spread[0, start:stop], deep, NT)
            total = first[:, :depth] + first[:, depth:]
            total = total + mm(spread[1, start:stop], deep_high, NT)
            for n, name in enumerate(names):
                tiles_of[name] = total[8 * n : 8 * n + 8]

        outer = [(x, a, t) for x in (rows_x, rows_x + 1, -1) for a in range(3) for t in (0, 1)]
        outer += [(x, a, 1) for x in range(rows_x) for a in range(3)]
        spread_tiles(outer, 0)
        for d, (sx, sy) in enumerate(DIRS):
            tiles = [
                tiles_of[x, a, 0 if sy == 0 else 1]
                for x in force_planes(sx, rows_x) for a in range(3)
            ]
            if sy:
                tiles = pack(tiles, 0 if sy == 1 else 7, 2 if sy == 1 else 1)
            for k, tile in enumerate(tiles):
                send_force[d][step, k] = tile
        launch(step, 0)
        spread_tiles([(x, a, 0) for x in range(rows_x) for a in range(3)], 8 * len(outer))

        @pl.when(step > 0)
        def _():
            finish_pops(step - 1)

        arrive(step, 0)
        parts = {(x, a): [tiles_of[x, a, 0]] for x in range(rows_x) for a in range(3)}
        for d, (sx, sy) in enumerate(DIRS):
            names = [
                (landing(x, sx, rows_x), a) for x in force_planes(sx, rows_x) for a in range(3)
            ]
            load = lambda k, d=d: recv_force[d][step, k]
            if sy == 0:
                tiles = [load(k) for k in range(len(names))]
            else:
                start, rows = (0, 2) if sy == 1 else (7, 1)
                mask = row_mask(start, rows, depth)
                tiles = [jnp.where(mask, t, 0.0) for t in unpack(load, len(names), rows)]
            for name, tile in zip(names, tiles):
                parts[name].append(tile)
        force = [
            jnp.stack([total_of(parts[x, a]) for x in range(rows_x)]) for a in range(3)
        ]

        relaxed = collide([pops_out[q] for q in range(19)], force, solid_ref[...] != 0)
        moved = [
            roll(roll(relaxed[q], VELOCITIES[q][2], 2), VELOCITIES[q][1], 1) for q in range(19)
        ]
        for q in range(19):
            moved_ref[q] = moved[q]
        nothing = jnp.zeros((1, 8, depth), jnp.float32)
        rho, mz = {}, {}
        for cx in (-1, 0, 1):
            for cy in (-1, 0, 1):
                members = [q for q in range(19) if VELOCITIES[q][:2] == (cx, cy)]
                pad = lambda v: jnp.concatenate(
                    [nothing] * (1 + cx) + [v] + [nothing] * (1 - cx), axis=0
                )
                rho[cx, cy] = pad(total_of([moved[q] for q in members]))
                up = [moved[q] for q in members if VELOCITIES[q][2] == 1]
                down = [moved[q] for q in members if VELOCITIES[q][2] == -1]
                if up:
                    mz[cx, cy] = pad(total_of(up) - total_of(down))
        first_row, last_row = sub == 0, sub == 7
        own = {}
        zero = jnp.zeros((rows_x + 2, 8, depth), jnp.float32)
        fields = []
        for cy in (0, 1, -1):
            dens = rho[-1, cy] + rho[0, cy] + rho[1, cy]
            deep_m = [mz[cx, cy] for cx in (-1, 0, 1) if (cx, cy) in mz]
            fields.append((
                dens, rho[1, cy] - rho[-1, cy], zero if cy == 0 else cy * dens, total_of(deep_m)
            ))
        for c in range(4):
            mid, up, down = (fields[g][c] for g in range(3))
            near = mid + jnp.where(first_row, 0.0, up) + jnp.where(last_row, 0.0, down)
            if c:
                half = 0.5 * force[c - 1]
                near = near + jnp.concatenate([nothing, half, nothing], axis=0)
            far = jnp.where(first_row, up, jnp.where(last_row, down, 0.0))
            for x in range(-1, rows_x + 1):
                own[x, c] = (near[x + 1], far[x + 1])
        for d, (sx, sy) in enumerate(DIRS):
            names = [(x, c) for x in moment_planes(sx, rows_x) for c in range(4)]
            near, far = [own[n][0] for n in names], [own[n][1] for n in names]
            if sy == 0:
                tiles = near + pack(far, 7, 2)
            elif sy == 1:
                tiles = pack([jnp.where(last_row, a, b) for a, b in zip(near, far)], 7, 2)
            else:
                tiles = pack(far, 7, 1) + pack(near, 0, 2)
            for k, tile in enumerate(tiles):
                send_mom[d][step, k] = tile
        launch(step, 1)
        for n, sx in enumerate((1, -1)):
            edge = rows_x - 1 if sx == 1 else 0
            for k, q in enumerate(XS[sx]):
                send_px[n][step, k] = moved[q][edge]
        for n, sy in enumerate((1, -1)):
            rows_kept = moved[YS[sy][0]]
            start = 0 if sy == 1 else 7
            for k, q in enumerate(YS[sy][1:], 1):
                rows_kept = jnp.where(sub == (start + k) % 8, roll(moved[q], k, 1), rows_kept)
            send_py[n][step] = rows_kept
        for n, (sx, sy) in enumerate(DIRS[4:]):
            send_pc[n][step] = moved[CORNER[sx, sy]][rows_x - 1 if sx == 1 else 0]
        launch(step, 2)
        arrive(step, 1)
        reach = [x for x in range(rows_x + 2)] + [-1]
        near = {(x, c): [] for x in reach for c in range(4)}
        far = {(x, c): [] for x in reach for c in range(4)}
        for name, (a, b) in own.items():
            near[name].append(a)
            far[name].append(b)
        two, edges, one = row_mask(0, 2, depth), row_mask(7, 2, depth), row_mask(7, 1, depth)
        for d, (sx, sy) in enumerate(DIRS):
            names = [
                (landing(x, sx, rows_x), c)
                for x in moment_planes(sx, rows_x) for c in range(4)
            ]
            count = len(names)
            load = lambda k, d=d: recv_mom[d][step, k]
            if sy == 0:
                a = [load(k) for k in range(count)]
                b = unpack(lambda k: load(count + k), count, 2)
                b = [jnp.where(edges, t, 0.0) for t in b]
            elif sy == 1:
                both_rows = unpack(load, count, 2)
                a = [jnp.where(first_row, t, 0.0) for t in both_rows]
                b = [jnp.where(last_row, t, 0.0) for t in both_rows]
            else:
                skip = packed(count, 1)
                a = [jnp.where(one, t, 0.0) for t in unpack(load, count, 1)]
                b = unpack(lambda k: load(skip + k), count, 2)
                b = [jnp.where(two, t, 0.0) for t in b]
            for name, p, r in zip(names, a, b):
                near[name].append(p)
                far[name].append(r)
        used = row_mask(7, 3, depth)
        for i, x in enumerate(reach):
            for t, side in enumerate((near, far)):
                dens = total_of(side[x, 0])
                if t:
                    dens = jnp.where(used, dens, 1.0)
                inverse = 1.0 / dens
                for a in range(3):
                    wide[i, a, t] = total_of(side[x, a + 1]) * inverse
        wide_high, wide_low = split(wide[...].reshape(planes * 3 * 16, depth))
        twice = jnp.concatenate([wide_high, wide_high], axis=1)
        along = mm(twice, deep, NN) + mm(wide_low, deep_high, NN)
        along = along.reshape(planes, 3, 16, vertices)
        drift, order = [], list(range(rows_x + 2)) + [7]
        for a in range(3):
            acc = along[0, a] * table_x[0:1]
            for i, x in enumerate(order[1:], 1):
                acc = acc + along[i, a] * table_x[x : x + 1]
            drift.append(jnp.sum(acc * table_y, axis=0, keepdims=True))
        off[...] = now + live * jnp.concatenate(drift, axis=0)
        return carry

    lax.fori_loop(0, SUBSTEPS, substep, 0)
    finish_pops(SUBSTEPS - 1)

    for m in range(slots):
        offset_out[:, m, :] = off[:, m * padded : (m + 1) * padded]

    def drain(step, carry):
        for stage in range(3):
            for x in copies(step, stage):
                x.wait_send()
        return carry

    lax.fori_loop(0, SUBSTEPS, drain, 0)


def local(mesh, populations, solid, base_cell, offset, rest, stiffness, occupied, triangles):
    rows_x, rows_y, depth = populations.shape[1:]
    slots, padded = offset.shape[3:]
    assert rows_y == 8 and rows_x == 4 and depth & (depth - 1) == 0
    vertices, planes, faces = slots * padded, rows_x + 3, triangles.shape[0]
    S = SUBSTEPS
    f32, bf16 = jnp.float32, jnp.bfloat16
    tile = (8, depth)
    pop_shapes = [(5,)] * 2 + [(rows_x,)] * 2 + [()] * 4
    V = lambda shape, dtype=f32: pltpu.VMEM(shape, dtype)
    scratch = [
        V((padded, faces), bf16), V((2, padded, padded), bf16), V((3, vertices)),
        V((2, planes * 48, vertices), bf16),
        V((19, rows_x) + tile), V((planes, 3, 2) + tile),
    ]
    for _ in ("receive", "send"):
        scratch += [V((S, force_size(*d, rows_x)) + tile) for d in DIRS]
        scratch += [V((S,) + p + tile) for p in pop_shapes]
        scratch += [V((S, moment_size(*d, rows_x)) + tile) for d in DIRS]
    scratch += [pltpu.SemaphoreType.DMA((S, 3, 8)), pltpu.SemaphoreType.DMA((S, 3, 8))]
    scratch += [pltpu.SemaphoreType.DMA(())]
    vmem = pl.BlockSpec(memory_space=pltpu.VMEM)
    smem = pl.BlockSpec(memory_space=pltpu.SMEM)
    small = (3, slots, padded)
    pops, moved = pl.pallas_call(
        functools.partial(body_kernel, mesh.shape["gx"], mesh.shape["gy"]),
        out_shape=(
            jax.ShapeDtypeStruct(populations.shape, f32),
            jax.ShapeDtypeStruct(small, f32),
        ),
        in_specs=[pl.BlockSpec(memory_space=pl.ANY)] + [vmem] * 4 + [smem] * 2 + [vmem],
        out_specs=(vmem, vmem),
        scratch_shapes=scratch,
        compiler_params=pltpu.CompilerParams(
            collective_id=0, has_side_effects=True, vmem_limit_bytes=60 * 1024 * 1024
        ),
    )(
        populations, solid, base_cell.reshape(small), offset.reshape(small), rest.reshape(small),
        stiffness.reshape(slots), occupied.reshape(slots), triangles.T,
    )
    return pops, moved.reshape(offset.shape)


def solution(mesh):
    in_specs = (
        P(None, "gx", "gy", None),
        P("gx", "gy", None),
        P(None, "gx", "gy", None, None),
        P(None, "gx", "gy", None, None),
        P(None, "gx", "gy", None, None),
        P("gx", "gy", None),
        P("gx", "gy", None),
        P(),
    )
    out_specs = (P(None, "gx", "gy", None), P(None, "gx", "gy", None, None))
    return jax.shard_map(
        functools.partial(local, mesh), mesh=mesh, in_specs=in_specs, out_specs=out_specs,
        check_vma=False,
    )
```

```python
import functools
import math

import jax
import jax.numpy as jnp
from jax import lax
from jax.experimental import pallas as pl
from jax.experimental.pallas import tpu as pltpu
from jax.sharding import PartitionSpec as P

SUBSTEPS = 3
VELOCITIES = [
    (0, 0, 0), (1, 0, 0), (-1, 0, 0), (0, 1, 0), (0, -1, 0), (0, 0, 1), (0, 0, -1),
    (1, 1, 0), (-1, -1, 0), (1, -1, 0), (-1, 1, 0), (1, 0, 1), (-1, 0, -1), (1, 0, -1),
    (-1, 0, 1), (0, 1, 1), (0, -1, -1), (0, 1, -1), (0, -1, 1),
]
OPPOSITE = [0, 2, 1, 4, 3, 6, 5, 8, 7, 10, 9, 12, 11, 14, 13, 16, 15, 18, 17]
LATTICE_WEIGHTS = [1.0 / 3.0] + [1.0 / 18.0] * 6 + [1.0 / 36.0] * 12
RELAX = 0.8
XS = {s: [q for q in range(19) if VELOCITIES[q][0] == s] for s in (1, -1)}
YS = {s: [q for q in range(19) if VELOCITIES[q][1] == s] for s in (1, -1)}
CORNER = {(v[0], v[1]): q for q, v in enumerate(VELOCITIES) if v[0] and v[1]}
DIRS = [(1, 0), (-1, 0), (0, 1), (0, -1), (1, 1), (1, -1), (-1, 1), (-1, -1)]
MESH = pl.DeviceIdType.MESH
NT = (((1,), (1,)), ((), ()))
NN = (((1,), (0,)), ((), ()))


def mm(a, b, dims):
    return lax.dot_general(a, b, dims, preferred_element_type=jnp.float32)


def split(value):
    high = value.astype(jnp.bfloat16)
    low = (value - high.astype(jnp.float32)).astype(jnp.bfloat16)
    return high, low


def quarter_sine(t):
    t = t - 4.0 * jnp.floor(t * 0.25 + 0.5)
    t = jnp.where(t > 1.0, 2.0 - t, jnp.where(t < -1.0, -2.0 - t, t))
    x = t * (math.pi / 2.0)
    u = x * x
    p = 1.0 / 6227020800.0
    for c in (-1.0 / 39916800.0, 1.0 / 362880.0, -1.0 / 5040.0, 1.0 / 120.0, -1.0 / 6.0, 1.0):
        p = p * u + c
    return x * p


def table(rows, base, kernels):
    cells = lax.broadcasted_iota(jnp.int32, (rows, base.shape[1]), 0)
    d = (cells - base + 1) & (rows - 1)
    out = jnp.where(d == 3, kernels[3], 0.0)
    for s in (2, 1, 0):
        out = jnp.where(d == s, kernels[s], out)
    return out


def moments(pops):
    density = functools.reduce(lambda a, b: a + b, pops)
    momentum = []
    for a in range(3):
        plus = [pops[q] for q in range(19) if VELOCITIES[q][a] == 1]
        minus = [pops[q] for q in range(19) if VELOCITIES[q][a] == -1]
        momentum.append(
            functools.reduce(lambda a, b: a + b, plus)
            - functools.reduce(lambda a, b: a + b, minus)
        )
    return density, momentum


def collide(pops, force, walled):
    density, momentum = moments(pops)
    inverse = 1.0 / density
    u = [(momentum[a] + 0.5 * force[a]) * inverse for a in range(3)]
    squared = u[0] * u[0] + u[1] * u[1] + u[2] * u[2]
    working = u[0] * force[0] + u[1] * force[1] + u[2] * force[2]
    base = 1.0 - 1.5 * squared
    relaxed = []
    for q in range(19):
        vector = VELOCITIES[q]
        along, pushed = jnp.zeros_like(density), jnp.zeros_like(density)
        for a in range(3):
            if vector[a] == 1:
                along, pushed = along + u[a], pushed + force[a]
            elif vector[a] == -1:
                along, pushed = along - u[a], pushed - force[a]
        w = LATTICE_WEIGHTS[q]
        equilibrium = (w * density) * (base + along * (3.0 + 4.5 * along))
        source = ((1.0 - 0.5 / RELAX) * w) * (3.0 * (pushed - working) + 9.0 * along * pushed)
        updated = pops[q] - (pops[q] - equilibrium) * (1.0 / RELAX) + source
        relaxed.append(jnp.where(walled, pops[OPPOSITE[q]], updated))
    return relaxed


def roll(x, shift, axis):
    size = x.shape[axis]
    shift = shift % size
    return x if shift == 0 else pltpu.roll(x, shift, axis)


def row_mask(start, rows, depth):
    sub = lax.broadcasted_iota(jnp.int32, (8, depth), 0)
    return ((sub - start) & 7) < rows


def pack(tiles, start, rows):
    per, out = 8 // rows, []
    for g in range(0, len(tiles), per):
        acc = tiles[g]
        for k, tile in enumerate(tiles[g + 1 : g + per], 1):
            mask = row_mask(start + k * rows, rows, tile.shape[1])
            acc = jnp.where(mask, roll(tile, k * rows, 0), acc)
        out.append(acc)
    return out


def unpack(load, count, rows):
    per = 8 // rows
    return [roll(load(k // per), -(k % per) * rows, 0) for k in range(count)]


def packed(count, rows):
    return -(-count // (8 // rows))


def force_planes(sx, rows_x):
    return {1: [rows_x, rows_x + 1], -1: [-1], 0: list(range(rows_x))}[sx]


def moment_planes(sx, rows_x):
    return {1: [rows_x - 1, rows_x], -1: [-1, 0, 1], 0: list(range(-1, rows_x + 1))}[sx]


def landing(x, sx, rows_x):
    return x - sx * rows_x


def force_size(sx, sy, rows_x):
    n = 3 * len(force_planes(sx, rows_x))
    return {0: n, 1: packed(n, 2), -1: packed(n, 1)}[sy]


def moment_size(sx, sy, rows_x):
    n = 4 * len(moment_planes(sx, rows_x))
    return {0: n + packed(n, 2), 1: packed(n, 2), -1: packed(n, 1) + packed(n, 2)}[sy]


def total_of(parts):
    return functools.reduce(lambda a, b: a + b, parts)


def body_kernel(
    peers_x, peers_y,
    pops_ref, solid_ref, base_ref, offset_ref, rest_ref, stiff_ref, occ_ref, tri_ref,
    pops_out, offset_out,
    lap, off, spread, moved_ref, wide,
    *scratch,
):
    recv_force, recv_pops, recv_mom = scratch[0:8], scratch[8:16], scratch[16:24]
    send_force, send_pops, send_mom = scratch[24:32], scratch[32:40], scratch[40:48]
    send_px, send_py, send_pc = send_pops[0:2], send_pops[2:4], send_pops[4:8]
    send_sem, recv_sem, load_sem = scratch[48:51]
    rows_x = pops_ref.shape[1]
    depth = pops_ref.shape[3]
    slots, padded = base_ref.shape[1], base_ref.shape[2]
    vertices = slots * padded
    planes = rows_x + 3
    ix, iy = lax.axis_index("gx"), lax.axis_index("gy")
    peer = [((ix + sx + peers_x) % peers_x, (iy + sy + peers_y) % peers_y) for sx, sy in DIRS]

    load_pops = pltpu.make_async_copy(pops_ref, pops_out, load_sem)
    load_pops.start()
    barrier = pltpu.get_barrier_semaphore()
    for p in peer:
        pl.semaphore_signal(barrier, inc=1, device_id=p, device_id_type=MESH)

    faces = tri_ref.shape[1]
    pairs = None
    for start in range(0, faces, 256):
        stop = min(start + 256, faces)
        ids = lax.broadcasted_iota(jnp.int32, (base_ref.shape[2], stop - start), 0)
        corner = [tri_ref[k : k + 1, start:stop] for k in range(3)]
        hit = (ids == corner[0]) | (ids == corner[1]) | (ids == corner[2])
        part = jnp.where(hit, 1.0, 0.0).astype(jnp.bfloat16)
        part = mm(part, part, NT)
        pairs = part if pairs is None else pairs + part
    same = lax.broadcasted_iota(jnp.int32, pairs.shape, 0) == lax.broadcasted_iota(
        jnp.int32, pairs.shape, 1
    )
    lap_high, lap_low = split(jnp.where(same, -2.0 * pairs, pairs))
    lap[0] = lap_high
    lap[1] = lap_low

    def flat(ref):
        return jnp.concatenate([ref[:, m, :] for m in range(slots)], axis=1)

    base = flat(base_ref)
    base_x = base[0:1] - ix * rows_x
    base_y = base[1:2] - iy * pops_ref.shape[2]
    base_z = base[2:3]
    live = jnp.concatenate(
        [jnp.full((1, padded), occ_ref[m].astype(jnp.float32)) for m in range(slots)], axis=1
    )
    scale = live * jnp.concatenate(
        [jnp.full((1, padded), stiff_ref[m]) for m in range(slots)], axis=1
    )
    off[...] = flat(offset_ref)
    sub = lax.broadcasted_iota(jnp.int32, (8, depth), 0)
    load_pops.wait()

    def copy(step, stage, d, src, dst):
        return pltpu.make_async_remote_copy(
            src_ref=src, dst_ref=dst.at[step], send_sem=send_sem.at[step, stage, d],
            recv_sem=recv_sem.at[step, stage, d], device_id=peer[d], device_id_type=MESH,
        )

    groups = ((send_force, recv_force), (send_mom, recv_mom), (send_pops, recv_pops))

    def copies(step, stage):
        src, dst = groups[stage]
        return [copy(step, stage, d, src[d].at[step], dst[d]) for d in range(8)]

    def launch(step, stage):
        sends = copies(step, stage)

        @pl.when(iy % 2 == 1)
        def _():
            for d in (4, 6, 2, 5, 7, 3, 0, 1):
                sends[d].start()

        @pl.when(iy % 2 == 0)
        def _():
            for d in (5, 7, 3, 4, 6, 2, 0, 1):
                sends[d].start()

    def arrive(step, stage):
        for x in copies(step, stage):
            x.wait_recv()

    def finish_pops(step):
        arrive(step, 2)
        from_y = {1: recv_pops[2][step], -1: recv_pops[3][step]}
        for q in range(19):
            sx, sy, _ = VELOCITIES[q]
            value = moved_ref[q]
            edge_row = sub == (0 if sy == 1 else 7)
            if sy:
                value = jnp.where(edge_row, roll(from_y[sy], -YS[sy].index(q), 1), value)
            if sx:
                side = recv_pops[0 if sx == 1 else 1][step, XS[sx].index(q)]
                if sy:
                    side = jnp.where(edge_row, recv_pops[DIRS.index((sx, sy))][step], side)
                if sx == 1:
                    value = jnp.concatenate([side[None], value[:-1]], axis=0)
                else:
                    value = jnp.concatenate([value[1:], side[None]], axis=0)
            pops_out[q] = value

    def substep(step, carry):
        now = off[...]
        strain = now - flat(rest_ref)
        six = jnp.concatenate(
            [strain[:, m * padded : (m + 1) * padded] for m in range(slots)], axis=0
        )
        six_high = six.astype(jnp.bfloat16).astype(jnp.float32)
        both = jnp.concatenate([six_high, six - six_high], axis=0).astype(jnp.bfloat16)
        pulled = mm(both, lap[0], NN) + mm(both, lap[1], NN)
        pulled = pulled[0 : 3 * slots] + pulled[3 * slots :]
        force_v = scale * jnp.concatenate(
            [pulled[3 * m : 3 * m + 3] for m in range(slots)], axis=1
        )
        s = quarter_sine(now) * 0.25
        c = quarter_sine(now + 1.0) * 0.25
        kernels = (0.25 - s, 0.25 + c, 0.25 + s, 0.25 - c)
        table_x = table(8, base_x, [k[0:1] for k in kernels])
        table_y = table(16, base_y, [k[1:2] for k in kernels])
        deep_high, deep_low = split(table(depth, base_z, [k[2:3] for k in kernels]))
        deep = jnp.concatenate([deep_high, deep_low], axis=0)
        tiles_of = {}

        def spread_tiles(names, start):
            for n in range(0, len(names), 2):
                blocks = [
                    (force_v[a : a + 1] * table_x[x & 7 : (x & 7) + 1])
                    * table_y[8 * t : 8 * t + 8]
                    for x, a, t in names[n : n + 2]
                ]
                high, low = split(jnp.concatenate(blocks, axis=0))
                row = start + 8 * n
                spread[0, row : row + 16, :] = high
                spread[1, row : row + 16, :] = low
            stop = start + 8 * len(names)
            first = mm(spread[0, start:stop], deep, NT)
            total = first[:, :depth] + first[:, depth:]
            total = total + mm(spread[1, start:stop], deep_high, NT)
            for n, name in enumerate(names):
                tiles_of[name] = total[8 * n : 8 * n + 8]

        outer = [(x, a, t) for x in (rows_x, rows_x + 1, -1) for a in range(3) for t in (0, 1)]
        outer += [(x, a, 1) for x in range(rows_x) for a in range(3)]
        spread_tiles(outer, 0)
        for d, (sx, sy) in enumerate(DIRS):
            tiles = [
                tiles_of[x, a, 0 if sy == 0 else 1]
                for x in force_planes(sx, rows_x) for a in range(3)
            ]
            if sy:
                tiles = pack(tiles, 0 if sy == 1 else 7, 2 if sy == 1 else 1)
            for k, tile in enumerate(tiles):
                send_force[d][step, k] = tile
        @pl.when(step == 0)
        def _():
            pl.semaphore_wait(barrier, len(peer))

        launch(step, 0)
        spread_tiles([(x, a, 0) for x in range(rows_x) for a in range(3)], 8 * len(outer))

        @pl.when(step > 0)
        def _():
            finish_pops(step - 1)

        arrive(step, 0)
        parts = {(x, a): [tiles_of[x, a, 0]] for x in range(rows_x) for a in range(3)}
        for d, (sx, sy) in enumerate(DIRS):
            names = [
                (landing(x, sx, rows_x), a) for x in force_planes(sx, rows_x) for a in range(3)
            ]
            load = lambda k, d=d: recv_force[d][step, k]
            if sy == 0:
                tiles = [load(k) for k in range(len(names))]
            else:
                start, rows = (0, 2) if sy == 1 else (7, 1)
                mask = row_mask(start, rows, depth)
                tiles = [jnp.where(mask, t, 0.0) for t in unpack(load, len(names), rows)]
            for name, tile in zip(names, tiles):
                parts[name].append(tile)
        force = [
            jnp.stack([total_of(parts[x, a]) for x in range(rows_x)]) for a in range(3)
        ]

        relaxed = collide([pops_out[q] for q in range(19)], force, solid_ref[...] != 0)
        moved = [
            roll(roll(relaxed[q], VELOCITIES[q][2], 2), VELOCITIES[q][1], 1) for q in range(19)
        ]
        for q in range(19):
            moved_ref[q] = moved[q]
        nothing = jnp.zeros((1, 8, depth), jnp.float32)
        rho, mz = {}, {}
        for cx in (-1, 0, 1):
            for cy in (-1, 0, 1):
                members = [q for q in range(19) if VELOCITIES[q][:2] == (cx, cy)]
                pad = lambda v: jnp.concatenate(
                    [nothing] * (1 + cx) + [v] + [nothing] * (1 - cx), axis=0
                )
                rho[cx, cy] = pad(total_of([moved[q] for q in members]))
                up = [moved[q] for q in members if VELOCITIES[q][2] == 1]
                down = [moved[q] for q in members if VELOCITIES[q][2] == -1]
                if up:
                    mz[cx, cy] = pad(total_of(up) - total_of(down))
        first_row, last_row = sub == 0, sub == 7
        own = {}
        zero = jnp.zeros((rows_x + 2, 8, depth), jnp.float32)
        fields = []
        for cy in (0, 1, -1):
            dens = rho[-1, cy] + rho[0, cy] + rho[1, cy]
            deep_m = [mz[cx, cy] for cx in (-1, 0, 1) if (cx, cy) in mz]
            fields.append((
                dens, rho[1, cy] - rho[-1, cy], zero if cy == 0 else cy * dens, total_of(deep_m)
            ))
        for c in range(4):
            mid, up, down = (fields[g][c] for g in range(3))
            near = mid + jnp.where(first_row, 0.0, up) + jnp.where(last_row, 0.0, down)
            if c:
                half = 0.5 * force[c - 1]
                near = near + jnp.concatenate([nothing, half, nothing], axis=0)
            far = jnp.where(first_row, up, jnp.where(last_row, down, 0.0))
            for x in range(-1, rows_x + 1):
                own[x, c] = (near[x + 1], far[x + 1])
        for d, (sx, sy) in enumerate(DIRS):
            names = [(x, c) for x in moment_planes(sx, rows_x) for c in range(4)]
            near, far = [own[n][0] for n in names], [own[n][1] for n in names]
            if sy == 0:
                tiles = near + pack(far, 7, 2)
            elif sy == 1:
                tiles = pack([jnp.where(last_row, a, b) for a, b in zip(near, far)], 7, 2)
            else:
                tiles = pack(far, 7, 1) + pack(near, 0, 2)
            for k, tile in enumerate(tiles):
                send_mom[d][step, k] = tile
        launch(step, 1)
        for n, sx in enumerate((1, -1)):
            edge = rows_x - 1 if sx == 1 else 0
            for k, q in enumerate(XS[sx]):
                send_px[n][step, k] = moved[q][edge]
        for n, sy in enumerate((1, -1)):
            rows_kept = moved[YS[sy][0]]
            start = 0 if sy == 1 else 7
            for k, q in enumerate(YS[sy][1:], 1):
                rows_kept = jnp.where(sub == (start + k) % 8, roll(moved[q], k, 1), rows_kept)
            send_py[n][step] = rows_kept
        for n, (sx, sy) in enumerate(DIRS[4:]):
            send_pc[n][step] = moved[CORNER[sx, sy]][rows_x - 1 if sx == 1 else 0]
        launch(step, 2)
        arrive(step, 1)
        reach = [x for x in range(rows_x + 2)] + [-1]
        near = {(x, c): [] for x in reach for c in range(4)}
        far = {(x, c): [] for x in reach for c in range(4)}
        for name, (a, b) in own.items():
            near[name].append(a)
            far[name].append(b)
        two, edges, one = row_mask(0, 2, depth), row_mask(7, 2, depth), row_mask(7, 1, depth)
        for d, (sx, sy) in enumerate(DIRS):
            names = [
                (landing(x, sx, rows_x), c)
                for x in moment_planes(sx, rows_x) for c in range(4)
            ]
            count = len(names)
            load = lambda k, d=d: recv_mom[d][step, k]
            if sy == 0:
                a = [load(k) for k in range(count)]
                b = unpack(lambda k: load(count + k), count, 2)
                b = [jnp.where(edges, t, 0.0) for t in b]
            elif sy == 1:
                both_rows = unpack(load, count, 2)
                a = [jnp.where(first_row, t, 0.0) for t in both_rows]
                b = [jnp.where(last_row, t, 0.0) for t in both_rows]
            else:
                skip = packed(count, 1)
                a = [jnp.where(one, t, 0.0) for t in unpack(load, count, 1)]
                b = unpack(lambda k: load(skip + k), count, 2)
                b = [jnp.where(two, t, 0.0) for t in b]
            for name, p, r in zip(names, a, b):
                near[name].append(p)
                far[name].append(r)
        used = row_mask(7, 3, depth)
        for i, x in enumerate(reach):
            for t, side in enumerate((near, far)):
                dens = total_of(side[x, 0])
                if t:
                    dens = jnp.where(used, dens, 1.0)
                inverse = 1.0 / dens
                for a in range(3):
                    wide[i, a, t] = total_of(side[x, a + 1]) * inverse
        wide_high, wide_low = split(wide[...].reshape(planes * 3 * 16, depth))
        twice = jnp.concatenate([wide_high, wide_high], axis=1)
        along = mm(twice, deep, NN) + mm(wide_low, deep_high, NN)
        along = along.reshape(planes, 3, 16, vertices)
        drift, order = [], list(range(rows_x + 2)) + [7]
        for a in range(3):
            acc = along[0, a] * table_x[0:1]
            for i, x in enumerate(order[1:], 1):
                acc = acc + along[i, a] * table_x[x : x + 1]
            drift.append(jnp.sum(acc * table_y, axis=0, keepdims=True))
        off[...] = now + live * jnp.concatenate(drift, axis=0)
        return carry

    lax.fori_loop(0, SUBSTEPS, substep, 0)
    finish_pops(SUBSTEPS - 1)

    for m in range(slots):
        offset_out[:, m, :] = off[:, m * padded : (m + 1) * padded]

    def drain(step, carry):
        for stage in range(3):
            for x in copies(step, stage):
                x.wait_send()
        return carry

    lax.fori_loop(0, SUBSTEPS, drain, 0)


def local(mesh, populations, solid, base_cell, offset, rest, stiffness, occupied, triangles):
    rows_x, rows_y, depth = populations.shape[1:]
    slots, padded = offset.shape[3:]
    assert rows_y == 8 and rows_x == 4 and depth & (depth - 1) == 0
    vertices, planes = slots * padded, rows_x + 3
    S = SUBSTEPS
    f32, bf16 = jnp.float32, jnp.bfloat16
    tile = (8, depth)
    pop_shapes = [(5,)] * 2 + [(rows_x,)] * 2 + [()] * 4
    V = lambda shape, dtype=f32: pltpu.VMEM(shape, dtype)
    scratch = [
        V((2, padded, padded), bf16), V((3, vertices)),
        V((2, planes * 48, vertices), bf16),
        V((19, rows_x) + tile), V((planes, 3, 2) + tile),
    ]
    for _ in ("receive", "send"):
        scratch += [V((S, force_size(*d, rows_x)) + tile) for d in DIRS]
        scratch += [V((S,) + p + tile) for p in pop_shapes]
        scratch += [V((S, moment_size(*d, rows_x)) + tile) for d in DIRS]
    scratch += [pltpu.SemaphoreType.DMA((S, 3, 8)), pltpu.SemaphoreType.DMA((S, 3, 8))]
    scratch += [pltpu.SemaphoreType.DMA(())]
    vmem = pl.BlockSpec(memory_space=pltpu.VMEM)
    smem = pl.BlockSpec(memory_space=pltpu.SMEM)
    small = (3, slots, padded)
    pops, moved = pl.pallas_call(
        functools.partial(body_kernel, mesh.shape["gx"], mesh.shape["gy"]),
        out_shape=(
            jax.ShapeDtypeStruct(populations.shape, f32),
            jax.ShapeDtypeStruct(small, f32),
        ),
        in_specs=[pl.BlockSpec(memory_space=pl.ANY)] + [vmem] * 4 + [smem] * 2 + [vmem],
        out_specs=(vmem, vmem),
        scratch_shapes=scratch,
        compiler_params=pltpu.CompilerParams(
            collective_id=0, has_side_effects=True, vmem_limit_bytes=60 * 1024 * 1024
        ),
    )(
        populations, solid, base_cell.reshape(small), offset.reshape(small), rest.reshape(small),
        stiffness.reshape(slots), occupied.reshape(slots), triangles.T,
    )
    return pops, moved.reshape(offset.shape)


def solution(mesh):
    in_specs = (
        P(None, "gx", "gy", None),
        P("gx", "gy", None),
        P(None, "gx", "gy", None, None),
        P(None, "gx", "gy", None, None),
        P(None, "gx", "gy", None, None),
        P("gx", "gy", None),
        P("gx", "gy", None),
        P(),
    )
    out_specs = (P(None, "gx", "gy", None), P(None, "gx", "gy", None, None))
    return jax.shard_map(
        functools.partial(local, mesh), mesh=mesh, in_specs=in_specs, out_specs=out_specs,
        check_vma=False,
    )
```

```python
import functools
import math

import jax
import jax.numpy as jnp
from jax import lax
from jax.experimental import pallas as pl
from jax.experimental.pallas import tpu as pltpu
from jax.sharding import PartitionSpec as P

SUBSTEPS = 3
VELOCITIES = [
    (0, 0, 0), (1, 0, 0), (-1, 0, 0), (0, 1, 0), (0, -1, 0), (0, 0, 1), (0, 0, -1),
    (1, 1, 0), (-1, -1, 0), (1, -1, 0), (-1, 1, 0), (1, 0, 1), (-1, 0, -1), (1, 0, -1),
    (-1, 0, 1), (0, 1, 1), (0, -1, -1), (0, 1, -1), (0, -1, 1),
]
OPPOSITE = [0, 2, 1, 4, 3, 6, 5, 8, 7, 10, 9, 12, 11, 14, 13, 16, 15, 18, 17]
LATTICE_WEIGHTS = [1.0 / 3.0] + [1.0 / 18.0] * 6 + [1.0 / 36.0] * 12
RELAX = 0.8
XS = {s: [q for q in range(19) if VELOCITIES[q][0] == s] for s in (1, -1)}
YS = {s: [q for q in range(19) if VELOCITIES[q][1] == s] for s in (1, -1)}
CORNER = {(v[0], v[1]): q for q, v in enumerate(VELOCITIES) if v[0] and v[1]}
DIRS = [(1, 0), (-1, 0), (0, 1), (0, -1), (1, 1), (1, -1), (-1, 1), (-1, -1)]
MESH = pl.DeviceIdType.MESH
NT = (((1,), (1,)), ((), ()))
NN = (((1,), (0,)), ((), ()))


def mm(a, b, dims):
    return lax.dot_general(a, b, dims, preferred_element_type=jnp.float32)


def split(value):
    high = value.astype(jnp.bfloat16)
    low = (value - high.astype(jnp.float32)).astype(jnp.bfloat16)
    return high, low


def quarter_sine(t):
    t = t - 4.0 * jnp.floor(t * 0.25 + 0.5)
    t = jnp.where(t > 1.0, 2.0 - t, jnp.where(t < -1.0, -2.0 - t, t))
    x = t * (math.pi / 2.0)
    u = x * x
    p = 1.0 / 6227020800.0
    for c in (-1.0 / 39916800.0, 1.0 / 362880.0, -1.0 / 5040.0, 1.0 / 120.0, -1.0 / 6.0, 1.0):
        p = p * u + c
    return x * p


def table(rows, base, kernels):
    cells = lax.broadcasted_iota(jnp.int32, (rows, base.shape[1]), 0)
    d = (cells - base + 1) & (rows - 1)
    out = jnp.where(d == 3, kernels[3], 0.0)
    for s in (2, 1, 0):
        out = jnp.where(d == s, kernels[s], out)
    return out


def moments(pops):
    density = functools.reduce(lambda a, b: a + b, pops)
    momentum = []
    for a in range(3):
        plus = [pops[q] for q in range(19) if VELOCITIES[q][a] == 1]
        minus = [pops[q] for q in range(19) if VELOCITIES[q][a] == -1]
        momentum.append(
            functools.reduce(lambda a, b: a + b, plus)
            - functools.reduce(lambda a, b: a + b, minus)
        )
    return density, momentum


def collide(pops, force, walled):
    density, momentum = moments(pops)
    inverse = 1.0 / density
    u = [(momentum[a] + 0.5 * force[a]) * inverse for a in range(3)]
    squared = u[0] * u[0] + u[1] * u[1] + u[2] * u[2]
    working = u[0] * force[0] + u[1] * force[1] + u[2] * force[2]
    base = 1.0 - 1.5 * squared
    relaxed = []
    for q in range(19):
        vector = VELOCITIES[q]
        along, pushed = jnp.zeros_like(density), jnp.zeros_like(density)
        for a in range(3):
            if vector[a] == 1:
                along, pushed = along + u[a], pushed + force[a]
            elif vector[a] == -1:
                along, pushed = along - u[a], pushed - force[a]
        w = LATTICE_WEIGHTS[q]
        equilibrium = (w * density) * (base + along * (3.0 + 4.5 * along))
        source = ((1.0 - 0.5 / RELAX) * w) * (3.0 * (pushed - working) + 9.0 * along * pushed)
        updated = pops[q] - (pops[q] - equilibrium) * (1.0 / RELAX) + source
        relaxed.append(jnp.where(walled, pops[OPPOSITE[q]], updated))
    return relaxed


def roll(x, shift, axis):
    size = x.shape[axis]
    shift = shift % size
    return x if shift == 0 else pltpu.roll(x, shift, axis)


def row_mask(start, rows, depth):
    sub = lax.broadcasted_iota(jnp.int32, (8, depth), 0)
    return ((sub - start) & 7) < rows


def pack(tiles, start, rows):
    per, out = 8 // rows, []
    for g in range(0, len(tiles), per):
        acc = tiles[g]
        for k, tile in enumerate(tiles[g + 1 : g + per], 1):
            mask = row_mask(start + k * rows, rows, tile.shape[1])
            acc = jnp.where(mask, roll(tile, k * rows, 0), acc)
        out.append(acc)
    return out


def unpack(load, count, rows):
    per = 8 // rows
    return [roll(load(k // per), -(k % per) * rows, 0) for k in range(count)]


def packed(count, rows):
    return -(-count // (8 // rows))


def force_planes(sx, rows_x):
    return {1: [rows_x, rows_x + 1], -1: [-1], 0: list(range(rows_x))}[sx]


def moment_planes(sx, rows_x):
    return {1: [rows_x - 1, rows_x], -1: [-1, 0, 1], 0: list(range(-1, rows_x + 1))}[sx]


def landing(x, sx, rows_x):
    return x - sx * rows_x


def force_size(sx, sy, rows_x):
    n = 3 * len(force_planes(sx, rows_x))
    return {0: n, 1: packed(n, 2), -1: packed(n, 1)}[sy]


def moment_size(sx, sy, rows_x):
    n = 4 * len(moment_planes(sx, rows_x))
    return {0: n + packed(n, 2), 1: packed(n, 2), -1: packed(n, 1) + packed(n, 2)}[sy]


def total_of(parts):
    return functools.reduce(lambda a, b: a + b, parts)


def body_kernel(
    peers_x, peers_y,
    pops_ref, solid_ref, base_ref, offset_ref, rest_ref, stiff_ref, occ_ref, tri_ref,
    pops_out, offset_out,
    lap, off, spread, moved_ref, wide,
    *scratch,
):
    recv_force, recv_pops, recv_mom = scratch[0:8], scratch[8:16], scratch[16:24]
    send_force, send_pops, send_mom = scratch[24:32], scratch[32:40], scratch[40:48]
    send_px, send_py, send_pc = send_pops[0:2], send_pops[2:4], send_pops[4:8]
    send_sem, recv_sem, load_sem = scratch[48:51]
    rows_x = pops_ref.shape[1]
    depth = pops_ref.shape[3]
    slots, padded = base_ref.shape[1], base_ref.shape[2]
    vertices = slots * padded
    planes = rows_x + 3
    ix, iy = lax.axis_index("gx"), lax.axis_index("gy")
    peer = [((ix + sx + peers_x) % peers_x, (iy + sy + peers_y) % peers_y) for sx, sy in DIRS]

    load_pops = pltpu.make_async_copy(pops_ref, pops_out, load_sem)
    load_pops.start()
    barrier = pltpu.get_barrier_semaphore()
    for p in peer:
        pl.semaphore_signal(barrier, inc=1, device_id=p, device_id_type=MESH)

    faces = tri_ref.shape[1]
    pairs = None
    for start in range(0, faces, 256):
        stop = min(start + 256, faces)
        ids = lax.broadcasted_iota(jnp.int32, (base_ref.shape[2], stop - start), 0)
        corner = [tri_ref[k : k + 1, start:stop] for k in range(3)]
        hit = (ids == corner[0]) | (ids == corner[1]) | (ids == corner[2])
        part = jnp.where(hit, 1.0, 0.0).astype(jnp.bfloat16)
        part = mm(part, part, NT)
        pairs = part if pairs is None else pairs + part
    same = lax.broadcasted_iota(jnp.int32, pairs.shape, 0) == lax.broadcasted_iota(
        jnp.int32, pairs.shape, 1
    )
    lap_high, lap_low = split(jnp.where(same, -2.0 * pairs, pairs))
    lap[0] = lap_high
    lap[1] = lap_low

    def flat(ref):
        return jnp.concatenate([ref[:, m, :] for m in range(slots)], axis=1)

    base = flat(base_ref)
    base_x = base[0:1] - ix * rows_x
    base_y = base[1:2] - iy * pops_ref.shape[2]
    base_z = base[2:3]
    live = jnp.concatenate(
        [jnp.full((1, padded), occ_ref[m].astype(jnp.float32)) for m in range(slots)], axis=1
    )
    scale = live * jnp.concatenate(
        [jnp.full((1, padded), stiff_ref[m]) for m in range(slots)], axis=1
    )
    off[...] = flat(offset_ref)
    sub = lax.broadcasted_iota(jnp.int32, (8, depth), 0)
    load_pops.wait()

    def copy(step, stage, d, src, dst):
        return pltpu.make_async_remote_copy(
            src_ref=src, dst_ref=dst.at[step], send_sem=send_sem.at[step, stage, d],
            recv_sem=recv_sem.at[step, stage, d], device_id=peer[d], device_id_type=MESH,
        )

    groups = ((send_force, recv_force), (send_mom, recv_mom), (send_pops, recv_pops))

    def copies(step, stage):
        src, dst = groups[stage]
        return [copy(step, stage, d, src[d].at[step], dst[d]) for d in range(8)]

    def launch(step, stage):
        sends = copies(step, stage)

        @pl.when(iy % 2 == 1)
        def _():
            for d in (4, 6, 2, 5, 7, 3, 0, 1):
                sends[d].start()

        @pl.when(iy % 2 == 0)
        def _():
            for d in (5, 7, 3, 4, 6, 2, 0, 1):
                sends[d].start()

    def arrive(step, stage):
        for x in copies(step, stage):
            x.wait_recv()

    def finish_pops(step):
        arrive(step, 2)
        from_y = {1: recv_pops[2][step], -1: recv_pops[3][step]}
        for q in range(19):
            sx, sy, _ = VELOCITIES[q]
            value = moved_ref[q]
            edge_row = sub == (0 if sy == 1 else 7)
            if sy:
                value = jnp.where(edge_row, roll(from_y[sy], -YS[sy].index(q), 1), value)
            if sx:
                side = recv_pops[0 if sx == 1 else 1][step, XS[sx].index(q)]
                if sy:
                    side = jnp.where(edge_row, recv_pops[DIRS.index((sx, sy))][step], side)
                if sx == 1:
                    value = jnp.concatenate([side[None], value[:-1]], axis=0)
                else:
                    value = jnp.concatenate([value[1:], side[None]], axis=0)
            pops_out[q] = value

    def substep(step, carry):
        now = off[...]
        strain = now - flat(rest_ref)
        six = jnp.concatenate(
            [strain[:, m * padded : (m + 1) * padded] for m in range(slots)], axis=0
        )
        six_high = six.astype(jnp.bfloat16).astype(jnp.float32)
        both = jnp.concatenate([six_high, six - six_high], axis=0).astype(jnp.bfloat16)
        pulled = mm(both, lap[0], NN) + mm(both, lap[1], NN)
        pulled = pulled[0 : 3 * slots] + pulled[3 * slots :]
        force_v = scale * jnp.concatenate(
            [pulled[3 * m : 3 * m + 3] for m in range(slots)], axis=1
        )
        s = quarter_sine(now) * 0.25
        c = quarter_sine(now + 1.0) * 0.25
        kernels = (0.25 - s, 0.25 + c, 0.25 + s, 0.25 - c)
        table_x = table(8, base_x, [k[0:1] for k in kernels])
        table_y = table(16, base_y, [k[1:2] for k in kernels])
        deep_high, deep_low = split(table(depth, base_z, [k[2:3] for k in kernels]))
        deep = jnp.concatenate([deep_high, deep_low], axis=0)
        tiles_of = {}

        def spread_tiles(names, start):
            for n in range(0, len(names), 2):
                blocks = [
                    (force_v[a : a + 1] * table_x[x & 7 : (x & 7) + 1])
                    * table_y[8 * t : 8 * t + 8]
                    for x, a, t in names[n : n + 2]
                ]
                high, low = split(jnp.concatenate(blocks, axis=0))
                row = start + 8 * n
                spread[0, row : row + 16, :] = high
                spread[1, row : row + 16, :] = low
            stop = start + 8 * len(names)
            first = mm(spread[0, start:stop], deep, NT)
            total = first[:, :depth] + first[:, depth:]
            total = total + mm(spread[1, start:stop], deep_high, NT)
            for n, name in enumerate(names):
                tiles_of[name] = total[8 * n : 8 * n + 8]

        outer = [(x, a, t) for x in (rows_x, rows_x + 1, -1) for a in range(3) for t in (0, 1)]
        outer += [(x, a, 1) for x in range(rows_x) for a in range(3)]
        spread_tiles(outer, 0)
        for d, (sx, sy) in enumerate(DIRS):
            tiles = [
                tiles_of[x, a, 0 if sy == 0 else 1]
                for x in force_planes(sx, rows_x) for a in range(3)
            ]
            if sy:
                tiles = pack(tiles, 0 if sy == 1 else 7, 2 if sy == 1 else 1)
            for k, tile in enumerate(tiles):
                send_force[d][step, k] = tile
        @pl.when(step == 0)
        def _():
            pl.semaphore_wait(barrier, len(peer))

        launch(step, 0)
        spread_tiles([(x, a, 0) for x in range(rows_x) for a in range(3)], 8 * len(outer))

        @pl.when(step > 0)
        def _():
            finish_pops(step - 1)

        arrive(step, 0)
        parts = {(x, a): [tiles_of[x, a, 0]] for x in range(rows_x) for a in range(3)}
        for d, (sx, sy) in enumerate(DIRS):
            names = [
                (landing(x, sx, rows_x), a) for x in force_planes(sx, rows_x) for a in range(3)
            ]
            load = lambda k, d=d: recv_force[d][step, k]
            if sy == 0:
                tiles = [load(k) for k in range(len(names))]
            else:
                start, rows = (0, 2) if sy == 1 else (7, 1)
                mask = row_mask(start, rows, depth)
                tiles = [jnp.where(mask, t, 0.0) for t in unpack(load, len(names), rows)]
            for name, tile in zip(names, tiles):
                parts[name].append(tile)
        force = [
            jnp.stack([total_of(parts[x, a]) for x in range(rows_x)]) for a in range(3)
        ]

        relaxed = collide([pops_out[q] for q in range(19)], force, solid_ref[...] != 0)
        moved = [
            roll(roll(relaxed[q], VELOCITIES[q][2], 2), VELOCITIES[q][1], 1) for q in range(19)
        ]
        for q in range(19):
            moved_ref[q] = moved[q]
        nothing = jnp.zeros((1, 8, depth), jnp.float32)
        rho, mz = {}, {}
        for cx in (-1, 0, 1):
            for cy in (-1, 0, 1):
                members = [q for q in range(19) if VELOCITIES[q][:2] == (cx, cy)]
                pad = lambda v: jnp.concatenate(
                    [nothing] * (1 + cx) + [v] + [nothing] * (1 - cx), axis=0
                )
                rho[cx, cy] = pad(total_of([moved[q] for q in members]))
                up = [moved[q] for q in members if VELOCITIES[q][2] == 1]
                down = [moved[q] for q in members if VELOCITIES[q][2] == -1]
                if up:
                    mz[cx, cy] = pad(total_of(up) - total_of(down))
        first_row, last_row = sub == 0, sub == 7
        own = {}
        zero = jnp.zeros((rows_x + 2, 8, depth), jnp.float32)
        fields = []
        for cy in (0, 1, -1):
            dens = rho[-1, cy] + rho[0, cy] + rho[1, cy]
            deep_m = [mz[cx, cy] for cx in (-1, 0, 1) if (cx, cy) in mz]
            fields.append((
                dens, rho[1, cy] - rho[-1, cy], zero if cy == 0 else cy * dens, total_of(deep_m)
            ))
        for c in range(4):
            mid, up, down = (fields[g][c] for g in range(3))
            near = mid + jnp.where(first_row, 0.0, up) + jnp.where(last_row, 0.0, down)
            if c:
                half = 0.5 * force[c - 1]
                near = near + jnp.concatenate([nothing, half, nothing], axis=0)
            far = jnp.where(first_row, up, jnp.where(last_row, down, 0.0))
            for x in range(-1, rows_x + 1):
                own[x, c] = (near[x + 1], far[x + 1])
        for d, (sx, sy) in enumerate(DIRS):
            names = [(x, c) for x in moment_planes(sx, rows_x) for c in range(4)]
            near, far = [own[n][0] for n in names], [own[n][1] for n in names]
            if sy == 0:
                tiles = near + pack(far, 7, 2)
            elif sy == 1:
                tiles = pack([jnp.where(last_row, a, b) for a, b in zip(near, far)], 7, 2)
            else:
                tiles = pack(far, 7, 1) + pack(near, 0, 2)
            for k, tile in enumerate(tiles):
                send_mom[d][step, k] = tile
        launch(step, 1)
        for n, sx in enumerate((1, -1)):
            edge = rows_x - 1 if sx == 1 else 0
            for k, q in enumerate(XS[sx]):
                send_px[n][step, k] = moved[q][edge]
        for n, sy in enumerate((1, -1)):
            rows_kept = moved[YS[sy][0]]
            start = 0 if sy == 1 else 7
            for k, q in enumerate(YS[sy][1:], 1):
                rows_kept = jnp.where(sub == (start + k) % 8, roll(moved[q], k, 1), rows_kept)
            send_py[n][step] = rows_kept
        for n, (sx, sy) in enumerate(DIRS[4:]):
            send_pc[n][step] = moved[CORNER[sx, sy]][rows_x - 1 if sx == 1 else 0]
        launch(step, 2)
        arrive(step, 1)
        reach = [x for x in range(rows_x + 2)] + [-1]
        near = {(x, c): [] for x in reach for c in range(4)}
        far = {(x, c): [] for x in reach for c in range(4)}
        for name, (a, b) in own.items():
            near[name].append(a)
            far[name].append(b)
        two, edges, one = row_mask(0, 2, depth), row_mask(7, 2, depth), row_mask(7, 1, depth)
        for d, (sx, sy) in enumerate(DIRS):
            names = [
                (landing(x, sx, rows_x), c)
                for x in moment_planes(sx, rows_x) for c in range(4)
            ]
            count = len(names)
            load = lambda k, d=d: recv_mom[d][step, k]
            if sy == 0:
                a = [load(k) for k in range(count)]
                b = unpack(lambda k: load(count + k), count, 2)
                b = [jnp.where(edges, t, 0.0) for t in b]
            elif sy == 1:
                both_rows = unpack(load, count, 2)
                a = [jnp.where(first_row, t, 0.0) for t in both_rows]
                b = [jnp.where(last_row, t, 0.0) for t in both_rows]
            else:
                skip = packed(count, 1)
                a = [jnp.where(one, t, 0.0) for t in unpack(load, count, 1)]
                b = unpack(lambda k: load(skip + k), count, 2)
                b = [jnp.where(two, t, 0.0) for t in b]
            for name, p, r in zip(names, a, b):
                near[name].append(p)
                far[name].append(r)
        used = row_mask(7, 3, depth)
        for i, x in enumerate(reach):
            for t, side in enumerate((near, far)):
                dens = total_of(side[x, 0])
                if t:
                    dens = jnp.where(used, dens, 1.0)
                inverse = 1.0 / dens
                for a in range(3):
                    wide[i, a, t] = total_of(side[x, a + 1]) * inverse
        wide_high, wide_low = split(wide[...].reshape(planes * 3 * 16, depth))
        twice = jnp.concatenate([wide_high, wide_high], axis=1)
        along = mm(twice, deep, NN) + mm(wide_low, deep_high, NN)
        along = along.reshape(planes, 3, 16, vertices)
        drift, order = [], list(range(rows_x + 2)) + [7]
        for a in range(3):
            acc = along[0, a] * table_x[0:1]
            for i, x in enumerate(order[1:], 1):
                acc = acc + along[i, a] * table_x[x : x + 1]
            drift.append(jnp.sum(acc * table_y, axis=0, keepdims=True))
        off[...] = now + live * jnp.concatenate(drift, axis=0)
        return carry

    lax.fori_loop(0, SUBSTEPS, substep, 0)
    finish_pops(SUBSTEPS - 1)

    for m in range(slots):
        offset_out[:, m, :] = off[:, m * padded : (m + 1) * padded] - offset_ref[:, m, :]

    def drain(step, carry):
        for stage in range(3):
            for x in copies(step, stage):
                x.wait_send()
        return carry

    lax.fori_loop(0, SUBSTEPS, drain, 0)


def local(mesh, populations, solid, base_cell, offset, rest, stiffness, occupied, triangles):
    rows_x, rows_y, depth = populations.shape[1:]
    slots, padded = offset.shape[3:]
    assert rows_y == 8 and rows_x == 4 and depth & (depth - 1) == 0
    vertices, planes = slots * padded, rows_x + 3
    S = SUBSTEPS
    f32, bf16 = jnp.float32, jnp.bfloat16
    tile = (8, depth)
    pop_shapes = [(5,)] * 2 + [(rows_x,)] * 2 + [()] * 4
    V = lambda shape, dtype=f32: pltpu.VMEM(shape, dtype)
    scratch = [
        V((2, padded, padded), bf16), V((3, vertices)),
        V((2, planes * 48, vertices), bf16),
        V((19, rows_x) + tile), V((planes, 3, 2) + tile),
    ]
    for _ in ("receive", "send"):
        scratch += [V((S, force_size(*d, rows_x)) + tile) for d in DIRS]
        scratch += [V((S,) + p + tile) for p in pop_shapes]
        scratch += [V((S, moment_size(*d, rows_x)) + tile) for d in DIRS]
    scratch += [pltpu.SemaphoreType.DMA((S, 3, 8)), pltpu.SemaphoreType.DMA((S, 3, 8))]
    scratch += [pltpu.SemaphoreType.DMA(())]
    vmem = pl.BlockSpec(memory_space=pltpu.VMEM)
    smem = pl.BlockSpec(memory_space=pltpu.SMEM)
    small = (3, slots, padded)
    pops, moved = pl.pallas_call(
        functools.partial(body_kernel, mesh.shape["gx"], mesh.shape["gy"]),
        out_shape=(
            jax.ShapeDtypeStruct(populations.shape, f32),
            jax.ShapeDtypeStruct(small, f32),
        ),
        in_specs=[pl.BlockSpec(memory_space=pl.ANY)] + [vmem] * 4 + [smem] * 2 + [vmem],
        out_specs=(vmem, vmem),
        scratch_shapes=scratch,
        compiler_params=pltpu.CompilerParams(
            collective_id=0, has_side_effects=True, vmem_limit_bytes=60 * 1024 * 1024
        ),
    )(
        populations, solid, base_cell.reshape(small), offset.reshape(small), rest.reshape(small),
        stiffness.reshape(slots), occupied.reshape(slots), triangles.T,
    )
    return pops, offset + moved.reshape(offset.shape)


def solution(mesh):
    in_specs = (
        P(None, "gx", "gy", None),
        P("gx", "gy", None),
        P(None, "gx", "gy", None, None),
        P(None, "gx", "gy", None, None),
        P(None, "gx", "gy", None, None),
        P("gx", "gy", None),
        P("gx", "gy", None),
        P(),
    )
    out_specs = (P(None, "gx", "gy", None), P(None, "gx", "gy", None, None))
    return jax.shard_map(
        functools.partial(local, mesh), mesh=mesh, in_specs=in_specs, out_specs=out_specs,
        check_vma=False,
    )
```
